8 devices in a mesh: ep: 8 (over z, y, x, core).
Axes of the slice: x: 2, y: 2, z: 1, core: 2. Of those that a mesh axis runs over, the one named last changes fastest.
Arguments:
- hidden: bfloat16 [1024, 1536], P('ep')
- grad_out: bfloat16 [1024, 1536], P('ep')
- w_router: bfloat16 [1536, 40], replicated
- b_router: float32 [40], replicated
- expert_ids: int32 [1024, 8], P('ep')
- slot_ids: int32 [1024, 8], P('ep')
- w_gate_up: bfloat16 [40, 1536, 1024], P('ep')
- b_gate_up: float32 [40, 1024], P('ep')
- w_down: bfloat16 [40, 512, 1536], P('ep')
- b_down: float32 [40, 1536], P('ep')
Outputs:
- output 1: bfloat16 [1024, 1536], P('ep')
- output 2: bfloat16 [1024, 1536], P('ep')
- output 3: float32 [1536, 40], replicated
- output 4: float32 [40], replicated
- output 5: float32 [40, 1536, 1024], P('ep')
- output 6: float32 [40, 1024], P('ep')
- output 7: float32 [40, 512, 1536], P('ep')
- output 8: float32 [40, 1536], P('ep')
All inputs are finite; a program needn't handle non-finite values.
Results may differ from the reference program's by a relative error of at most 0.0050715.
Values are sent between devices in bfloat16 or wider.
A program may use at most 1 GiB of HBM per device.

```python
import jax
import jax.numpy as jnp
from jax import lax

D_MODEL = 1536
FF_EXPERT = 512
EXPERTS = 40
TOP_K = 8
TOKENS_DEV = 128
EP_DEVICES = 8

TOKENS = EP_DEVICES * TOKENS_DEV
CAPACITY = (3 * TOKENS_DEV * TOP_K + 2 * EXPERTS - 1) // (2 * EXPERTS)
ROWS_EXPERT = EP_DEVICES * CAPACITY
SWIGLU_LIMIT = 7.0
SWIGLU_ALPHA = 1.702


def draw_routing(key):
    key_bias, key_dev = jax.random.split(key)
    expert_bias = jax.random.randint(key_bias, (EXPERTS,), 0, 512)
    expert_range = jnp.arange(EXPERTS, dtype=jnp.int32)
    copies = TOKENS_DEV * TOP_K

    def one_device(dev_key):
        key_noise, key_hot, key_pick, key_prio = jax.random.split(dev_key, 4)
        noise_int = jax.random.randint(key_noise, (TOKENS_DEV, EXPERTS), 0, 1024)
        hot_expert = jax.random.randint(key_hot, (), 0, EXPERTS)
        forced = jax.random.permutation(key_pick, TOKENS_DEV) < 2 * CAPACITY
        hot_bonus = jnp.where(forced[:, None] & (expert_range[None, :] == hot_expert), 4096, 0)
        scores = (noise_int + expert_bias[None, :] + hot_bonus) * EXPERTS + expert_range[None, :]
        choice = lax.top_k(scores, TOP_K)[1].astype(jnp.int32)
        flat_ids = choice.reshape(-1)
        priority = jax.random.permutation(key_prio, copies)
        sort_order = jnp.argsort(flat_ids * copies + priority)
        counts = jnp.bincount(flat_ids, length=EXPERTS)
        starts = jnp.cumsum(counts) - counts
        rank_sorted = (jnp.arange(copies, dtype=jnp.int32) - starts[flat_ids[sort_order]]).astype(jnp.int32)
        slot_rank = jnp.zeros((copies,), jnp.int32).at[sort_order].set(rank_sorted)
        slot_ids = jnp.where(slot_rank < CAPACITY, slot_rank, -1).reshape(TOKENS_DEV, TOP_K)
        return choice, slot_ids

    choice, slot_ids = jax.vmap(one_device)(jax.random.split(key_dev, EP_DEVICES))
    return choice.reshape(TOKENS, TOP_K), slot_ids.reshape(TOKENS, TOP_K).astype(jnp.int32)


def setup_inputs(seed: int = 0) -> dict:
    key_list = jax.random.split(jax.random.key(seed), 9)
    hidden = jax.random.normal(key_list[0], (TOKENS, D_MODEL), jnp.float32).astype(jnp.bfloat16)
    grad_out = jax.random.normal(key_list[1], (TOKENS, D_MODEL), jnp.float32).astype(jnp.bfloat16)
    w_router = (2.0 * D_MODEL ** -0.5 * jax.random.normal(key_list[2], (D_MODEL, EXPERTS), jnp.float32)).astype(jnp.bfloat16)
    b_router = jax.random.normal(key_list[3], (EXPERTS,), jnp.float32)
    expert_ids, slot_ids = draw_routing(key_list[4])
    w_gate_up = (3.0 * D_MODEL ** -0.5 * jax.random.normal(key_list[5], (EXPERTS, D_MODEL, 2 * FF_EXPERT), jnp.float32)).astype(jnp.bfloat16)
    b_gate_up = jax.random.normal(key_list[6], (EXPERTS, 2 * FF_EXPERT), jnp.float32)
    w_down = (0.15 * FF_EXPERT ** -0.5 * jax.random.normal(key_list[7], (EXPERTS, FF_EXPERT, D_MODEL), jnp.float32)).astype(jnp.bfloat16)
    b_down = 0.5 * jax.random.normal(key_list[8], (EXPERTS, D_MODEL), jnp.float32)
    return {'hidden': hidden, 'grad_out': grad_out, 'w_router': w_router, 'b_router': b_router, 'expert_ids': expert_ids, 'slot_ids': slot_ids, 'w_gate_up': w_gate_up, 'b_gate_up': b_gate_up, 'w_down': w_down, 'b_down': b_down}


def swiglu(pre_act):
    col_pairs = pre_act.reshape(pre_act.shape[:-1] + (pre_act.shape[-1] // 2, 2))
    gate_in = jnp.minimum(col_pairs[..., 0], SWIGLU_LIMIT)
    up_in = jnp.clip(col_pairs[..., 1], -SWIGLU_LIMIT, SWIGLU_LIMIT)
    return gate_in * jax.nn.sigmoid(SWIGLU_ALPHA * gate_in) * (up_in + 1.0)


def reference(hidden, grad_out, w_router, b_router, expert_ids, slot_ids, w_gate_up, b_gate_up, w_down, b_down):
    buf_total = EXPERTS * ROWS_EXPERT
    copy_count = TOKENS * TOP_K
    src_dev = (jnp.arange(TOKENS, dtype=jnp.int32) // TOKENS_DEV)[:, None]
    dest_row = jnp.where(slot_ids >= 0, expert_ids * ROWS_EXPERT + src_dev * CAPACITY + slot_ids, buf_total)
    src_copy = jnp.full((buf_total + 1,), copy_count, jnp.int32).at[dest_row.reshape(-1)].set(jnp.arange(copy_count, dtype=jnp.int32))[:buf_total].reshape(EXPERTS, ROWS_EXPERT)
    logits = jnp.dot(hidden, w_router, preferred_element_type=jnp.float32) + b_router
    gate_w = jax.nn.softmax(jnp.take_along_axis(logits, expert_ids, axis=1), axis=-1)
    flat_gate = gate_w.reshape(-1)

    def expert_forward(expert_args):
        w_gu, b_gu, w_dn, b_dn, src_rows = expert_args
        x_rows = jnp.take(hidden, src_rows // TOP_K, axis=0, mode='fill', fill_value=0)
        pre_act = jnp.dot(x_rows, w_gu, preferred_element_type=jnp.float32) + b_gu
        act_bf = swiglu(pre_act).astype(jnp.bfloat16)
        return (jnp.dot(act_bf, w_dn, preferred_element_type=jnp.float32) + b_dn).astype(jnp.bfloat16)

    y_flat = lax.map(expert_forward, (w_gate_up, b_gate_up, w_down, b_down, src_copy)).reshape(buf_total, D_MODEL)

    def token_forward(block_args):
        gate_blk, dest_blk, grad_blk = block_args
        y_blk = jnp.take(y_flat, dest_blk, axis=0, mode='fill', fill_value=0).astype(jnp.float32)
        out_blk = jnp.sum(gate_blk[:, :, None] * y_blk, axis=1).astype(jnp.bfloat16)
        return out_blk, jnp.einsum('td,tkd->tk', grad_blk.astype(jnp.float32), y_blk)

    dev_shape = (EP_DEVICES, TOKENS_DEV)
    block_out, gate_grad = lax.map(token_forward, (gate_w.reshape(dev_shape + (TOP_K,)), dest_row.reshape(dev_shape + (TOP_K,)), grad_out.reshape(dev_shape + (D_MODEL,))))
    block_out = block_out.reshape(TOKENS, D_MODEL)
    gate_grad = gate_grad.reshape(TOKENS, TOP_K)
    sel_grad = gate_w * (gate_grad - jnp.sum(gate_w * gate_grad, axis=1, keepdims=True))
    logit_grad = jnp.zeros((TOKENS, EXPERTS), jnp.float32).at[jnp.arange(TOKENS)[:, None], expert_ids].add(sel_grad).astype(jnp.bfloat16)

    def expert_backward(expert_args):
        w_gu, b_gu, w_dn, src_rows = expert_args
        tok_rows = src_rows // TOP_K
        x_rows = jnp.take(hidden, tok_rows, axis=0, mode='fill', fill_value=0)
        pre_act = jnp.dot(x_rows, w_gu, preferred_element_type=jnp.float32) + b_gu
        act_val, act_vjp = jax.vjp(swiglu, pre_act)
        act_bf = act_val.astype(jnp.bfloat16)
        row_gate = jnp.take(flat_gate, src_rows, axis=0, mode='fill', fill_value=0)
        row_grad = jnp.take(grad_out, tok_rows, axis=0, mode='fill', fill_value=0).astype(jnp.float32)
        q_rows = (row_gate[:, None] * row_grad).astype(jnp.bfloat16)
        grad_b_dn = jnp.sum(q_rows.astype(jnp.float32), axis=0)
        grad_w_dn = jnp.dot(act_bf.T, q_rows, preferred_element_type=jnp.float32)
        act_grad = jnp.dot(q_rows, w_dn.T, preferred_element_type=jnp.float32)
        pre_grad = act_vjp(act_grad)[0].astype(jnp.bfloat16)
        grad_b_gu = jnp.sum(pre_grad.astype(jnp.float32), axis=0)
        grad_w_gu = jnp.dot(x_rows.T, pre_grad, preferred_element_type=jnp.float32)
        p_rows = jnp.dot(pre_grad, w_gu.T, preferred_element_type=jnp.float32).astype(jnp.bfloat16)
        return grad_w_gu, grad_b_gu, grad_w_dn, grad_b_dn, p_rows

    grad_w_gate_up, grad_b_gate_up, grad_w_down, grad_b_down, p_rows = lax.map(expert_backward, (w_gate_up, b_gate_up, w_down, src_copy))
    p_flat = p_rows.reshape(buf_total, D_MODEL)

    def token_backward(block_args):
        dest_blk, logit_blk = block_args
        p_blk = jnp.take(p_flat, dest_blk, axis=0, mode='fill', fill_value=0).astype(jnp.float32)
        router_dx = jnp.dot(logit_blk, w_router.T, preferred_element_type=jnp.float32)
        return (jnp.sum(p_blk, axis=1) + router_dx).astype(jnp.bfloat16)

    grad_hidden = lax.map(token_backward, (dest_row.reshape(dev_shape + (TOP_K,)), logit_grad.reshape(dev_shape + (EXPERTS,)))).reshape(TOKENS, D_MODEL)
    grad_w_router = jnp.dot(hidden.T, logit_grad, preferred_element_type=jnp.float32)
    grad_b_router = jnp.sum(logit_grad.astype(jnp.float32), axis=0)
    return (block_out, grad_hidden, grad_w_router, grad_b_router, grad_w_gate_up, grad_b_gate_up, grad_w_down, grad_b_down)
```

```python
import functools

import jax
import jax.numpy as jnp
from jax import lax
from jax.experimental import pallas as pl
from jax.experimental.pallas import tpu as pltpu
from jax.sharding import PartitionSpec as P

LIMIT = 7.0
ALPHA = 1.702

CH = 4
EX = 40
NE = 5
TD = 128
D = 1536
F = 512
SL = 40
R2 = 2 * SL
RE = CH * R2
SP = 48
KC = NE * SP
TK = 8
BF = jnp.bfloat16
F32 = jnp.float32
ANY = pl.BlockSpec(memory_space=pl.ANY)
VM = pl.BlockSpec(memory_space=pltpu.VMEM)
VLIMIT = 67000000


def dot_nn(a, b):
    return lax.dot_general(a, b, (((1,), (0,)), ((), ())), preferred_element_type=F32)


def dot_nt(a, b):
    return lax.dot_general(a, b, (((1,), (1,)), ((), ())), preferred_element_type=F32)


def dot_tn(a, b):
    return lax.dot_general(a, b, (((0,), (0,)), ((), ())), preferred_element_type=F32)


def deinterleave_matrix():
    row = lax.broadcasted_iota(jnp.int32, (256, 256), 0)
    col = lax.broadcasted_iota(jnp.int32, (256, 256), 1)
    src = jnp.where(col < 128, 2 * col, 2 * col - 255)
    return jnp.where(row == src, 1.0, 0.0).astype(BF)


def entry_barrier(peers):
    barrier = pltpu.get_barrier_semaphore()
    for p in peers:
        pl.semaphore_signal(barrier, inc=1, device_id=(p,), device_id_type=pl.DeviceIdType.MESH)
    pl.semaphore_wait(barrier, len(peers))


def remote(src, dst, ssem, rsem, dev):
    return pltpu.make_async_remote_copy(src_ref=src, dst_ref=dst, send_sem=ssem, recv_sem=rsem,
                                        device_id=(dev,), device_id_type=pl.DeviceIdType.MESH)


class Gather:
    def __init__(self, me, own, buf, ssem, rsem):
        self.me, self.own, self.buf, self.ssem, self.rsem = me, own, buf, ssem, rsem

    def block(self, dev, lo=0, n=TD):
        core = lax.rem(dev, 2)
        return self.buf.at[dev // 2, pl.ds(pl.multiple_of(core * TD + lo, 64), n), :]

    def copy(self, slot, src, dst, dev):
        return remote(src, dst, self.ssem.at[slot], self.rsem.at[slot], dev)

    def descs(self):
        me = self.me
        c, x, y = me ^ 1, me ^ 2, me ^ 4
        own, blk, cp = self.own, self.block, self.copy
        self.x0 = cp(0, own.at[pl.ds(0, 64), :], blk(me, 0, 64), x)
        self.x1 = cp(1, own.at[pl.ds(64, 64), :], blk(me, 64, 64), x)
        self.y0 = cp(2, own.at[pl.ds(0, 64), :], blk(me, 0, 64), y)
        self.y1 = cp(3, own.at[pl.ds(64, 64), :], blk(me, 64, 64), y)
        self.d0 = cp(4, blk(x, 0, 64), blk(x, 0, 64), y)
        self.d1 = cp(5, blk(y, 64, 64), blk(y, 64, 64), x)
        self.c0 = cp(6, own, blk(me), c)
        self.c1 = cp(7, blk(x), blk(x), c)
        self.c2 = cp(8, blk(y), blk(y), c)
        self.c3 = cp(9, blk(me ^ 6), blk(me ^ 6), c)

    def start_own(self):
        self.descs()
        self.x0.start()
        self.y1.start()
        self.c0.start()
        self.x1.start()
        self.y0.start()

    def relay(self):
        self.x0.wait_recv()
        self.d0.start()
        self.y1.wait_recv()
        self.d1.start()

    def pair_xy(self):
        self.x1.wait_recv()
        self.c1.start()
        self.y0.wait_recv()
        self.c2.start()

    def pair_d(self):
        self.d0.wait_recv()
        self.d1.wait_recv()
        self.c3.start()

    def drain_sends(self):
        for d in (self.x0, self.x1, self.y0, self.y1, self.d0, self.d1, self.c0, self.c1, self.c2, self.c3):
            d.wait_send()


def split3(v):
    hi = v.astype(BF)
    r1 = v - hi.astype(F32)
    mid = r1.astype(BF)
    lo = (r1 - mid.astype(F32)).astype(BF)
    return hi, mid, lo


def forward_kernel(x_hbm, dy_hbm, meta_hbm, wrt_ref, br_ref, bgu_ref, bd_ref, wgu_hbm, wd_hbm,
                   sA, sB, kA, kB, xall_hbm, dyall_hbm, X_hbm, h_hbm, A_hbm, Y_hbm,
                   p_out, p48_out, wt_out, wloc_out,
                   xall, dyall, meta, wgu, wd, X, Y, YQ, h, A, pw, snd, rcv, perm,
                   lsem, wsem, osem, xs, xr, ds, dr, ms, mr, cs, cr):
    me = lax.axis_index('ep')
    chip = me // 2
    core = lax.rem(me, 2)
    for e in range(NE):
        pltpu.make_async_copy(wgu_hbm.at[e], wgu.at[e], wsem.at[e]).start()
    own_x = pltpu.make_async_copy(x_hbm, xall.at[chip, pl.ds(pl.multiple_of(core * TD, TD), TD), :], lsem.at[0])
    own_dy = pltpu.make_async_copy(dy_hbm, dyall.at[chip, pl.ds(pl.multiple_of(core * TD, TD), TD), :], lsem.at[1])
    own_m = pltpu.make_async_copy(meta_hbm, meta.at[me], lsem.at[2])
    own_x.start()
    own_dy.start()
    own_m.start()
    entry_barrier([me ^ m for m in range(1, 8)])
    gx = Gather(me, x_hbm, xall, xs, xr)
    gy = Gather(me, dy_hbm, dyall, ds, dr)
    metas = [remote(meta_hbm, meta.at[me], ms.at[m - 1], mr.at[m - 1], me ^ m) for m in range(1, 8)]
    for c in metas:
        c.start()
    gx.start_own()
    for e in range(NE):
        pltpu.make_async_copy(wd_hbm.at[e], wd.at[e], wsem.at[NE + e]).start()
    perm[...] = deinterleave_matrix()
    YQ[...] = jnp.zeros_like(YQ)
    pw[...] = jnp.zeros_like(pw)
    p48_out[...] = jnp.zeros_like(p48_out)

    def permute(e):
        pltpu.make_async_copy(wgu_hbm.at[e], wgu.at[e], wsem.at[e]).wait()

        def body(i, _):
            r = i // 4
            b = lax.rem(i, 4)
            rows = pl.ds(pl.multiple_of(r * 512, 512), 512)
            cols = pl.ds(pl.multiple_of(b * 256, 256), 256)
            wgu[e, rows, cols] = dot_nn(wgu[e, rows, cols], perm[...]).astype(BF)
            return 0

        lax.fori_loop(0, 12, body, 0)

    permute(0)
    permute(1)
    gx.relay()
    gy.start_own()
    permute(2)
    permute(3)
    own_x.wait()
    own_m.wait()
    for c in metas:
        c.wait()
    permute(4)

    iota40 = lax.broadcasted_iota(jnp.int32, (EX, TD), 0)
    iota80 = lax.broadcasted_iota(jnp.int32, (R2, 2 * TD), 0)
    iota48 = lax.broadcasted_iota(jnp.int32, (SP, TD), 0)

    def route(q):
        lt = dot_nt(wrt_ref[...], xall[q]) + br_ref[...]
        slots, gates = [], []
        for k in range(2):
            ids = meta[2 * q + k, 0:TK, :]
            slt = meta[2 * q + k, TK:2 * TK, :]
            slot = jnp.full((EX, TD), -1, jnp.int32)
            chosen = jnp.zeros((EX, TD), jnp.int32)
            for j in range(TK):
                hit = ids[j:j + 1, :] == iota40
                slot = jnp.where(hit, slt[j:j + 1, :], slot)
                chosen = jnp.where(hit, 1, chosen)
            on = chosen == 1
            lk = lt[:, k * TD:(k + 1) * TD]
            mx = jnp.max(jnp.where(on, lk, -jnp.inf), axis=0, keepdims=True)
            ex = jnp.where(on, jnp.exp(lk - mx), 0.0)
            w = ex / jnp.sum(ex, axis=0, keepdims=True)
            wt_out[2 * q + k] = w
            slots.append(slot)
            gates.append(w)
        for i in range(NE):
            mine = iota40 == me * NE + i
            codes = []
            ws = []
            for k in range(2):
                s = jnp.max(jnp.where(mine, slots[k].astype(F32), -1.0), axis=0, keepdims=True)
                wv = jnp.sum(jnp.where(mine, gates[k], 0.0), axis=0, keepdims=True)
                s = s.astype(jnp.int32)
                hot = s == iota48
                p48_out[2 * q + k, i * SP:(i + 1) * SP, :] = jnp.where(hot, 1.0, 0.0).astype(BF)
                for n, part in enumerate(split3(jnp.where(hot, wv, 0.0))):
                    pw[2 * q + k, i * SP:(i + 1) * SP, n * TD:(n + 1) * TD] = part
                codes.append(jnp.where(s >= 0, s + SL * k, -1))
                ws.append(wv)
            code = jnp.concatenate(codes, axis=1)
            wloc_out[q, i:i + 1, :] = jnp.concatenate(ws, axis=1)
            p_out[q, i * R2:(i + 1) * R2, :] = jnp.where(iota80 == code, 1.0, 0.0).astype(BF)
        for nb in range(3):
            cols = slice(nb * 512, nb * 512 + 512)
            rows = dot_nn(p_out[q], xall[q, :, cols])
            for i in range(NE):
                X[i, pl.ds(pl.multiple_of(q * R2, R2), R2), cols] = rows[i * R2:(i + 1) * R2].astype(BF)

    gx.c0.wait_recv()
    wloc_out[...] = jnp.zeros_like(wloc_out)
    route(chip)
    gx.pair_xy()
    gx.pair_d()
    gx.c1.wait_recv()
    gx.c2.wait_recv()

    def route_next(i, _):
        route(chip ^ i)
        return 0

    lax.fori_loop(1, 3, route_next, 0)
    gx.c3.wait_recv()
    route(chip ^ 3)
    out_x = pltpu.make_async_copy(xall, xall_hbm, osem.at[0])
    out_x.start()

    def expert(e):
        pltpu.make_async_copy(wd_hbm.at[e], wd.at[e], wsem.at[NE + e]).wait()
        slot = e % 2
        oh = pltpu.make_async_copy(h.at[slot], h_hbm.at[e], osem.at[2 + slot])
        oy = pltpu.make_async_copy(Y.at[slot], Y_hbm.at[e], osem.at[4 + slot])
        if e >= 2:
            oh.wait()
            oy.wait()

        def gate_up(b, _):
            cols = pl.ds(pl.multiple_of(b * 256, 256), 256)
            pre = dot_nn(X[e], wgu[e, :, cols]) + bgu_ref[e, :, cols]
            h[slot, :, cols] = pre
            g = jnp.minimum(pre[:, :128], LIMIT)
            u = jnp.clip(pre[:, 128:], -LIMIT, LIMIT)
            act = g * jax.nn.sigmoid(ALPHA * g) * (u + 1.0)
            A[e, :, pl.ds(pl.multiple_of(b * 128, 128), 128)] = act.astype(BF)
            return 0

        lax.fori_loop(0, 4, gate_up, 0)
        oh.start()

        def down(b, _):
            cols = pl.ds(pl.multiple_of(b * 512, 512), 512)
            y = dot_nn(A[e], wd[e, :, cols]) + bd_ref[e, :, cols]
            Y[slot, :, cols] = y.astype(BF)
            for q in range(2 * CH):
                YQ[q, e * SP:e * SP + SL, cols] = y[q * SL:(q + 1) * SL].astype(BF)
            return 0

        lax.fori_loop(0, 3, down, 0)
        oy.start()

    expert(0)
    gy.relay()
    expert(1)
    expert(2)
    gy.pair_xy()
    expert(3)
    expert(4)
    gy.pair_d()
    out_X = pltpu.make_async_copy(X, X_hbm, osem.at[6])
    out_A = pltpu.make_async_copy(A, A_hbm, osem.at[7])
    out_X.start()
    out_A.start()

    def combine(dev, dst):
        for nb in range(3):
            cols = slice(nb * 512, nb * 512 + 512)
            full = dot_tn(pw[dev], YQ[dev, :, cols])
            dst[:, cols] = full[0:TD] + full[TD:2 * TD] + full[2 * TD:3 * TD]

    exchange(me, combine, snd, rcv, cs, cr, sA, sB, kA, kB, osem, 8)

    gy.c0.wait_recv()
    gy.c1.wait_recv()
    gy.c2.wait_recv()
    gy.c3.wait_recv()
    own_dy.wait()
    out_dy = pltpu.make_async_copy(dyall, dyall_hbm, osem.at[1])
    out_dy.start()
    for e in (3, 4):
        pltpu.make_async_copy(h.at[e % 2], h_hbm.at[e], osem.at[2 + e % 2]).wait()
        pltpu.make_async_copy(Y.at[e % 2], Y_hbm.at[e], osem.at[4 + e % 2]).wait()
    out_x.wait()
    out_X.wait()
    out_A.wait()
    out_dy.wait()
    gx.drain_sends()
    gy.drain_sends()


def exchange(me, combine, snd, rcv, cs, cr, sA, sB, kA, kB, osem, base):
    order = (3, 1, 2, 0)
    copies = [remote(snd.at[n], rcv.at[n], cs.at[n], cr.at[n], me ^ 1) for n in range(CH)]

    for n, rel in enumerate(order):
        combine(me ^ 1 ^ (2 * rel), snd.at[n])
        if n:
            copies[n - 1].start()
    outs = []
    half = D // 2
    places = {3: ((sA, 1), (sB, 1)), 1: ((sA, 0), (kB, 1)), 2: ((kA, 1), (sB, 0)), 0: ((kA, 0), (kB, 0))}
    for n, rel in enumerate(order):
        if n == 1:
            copies[CH - 1].start()

        def add_block(dst, n=n):
            return dst

        acc = _Acc(rcv.at[n])
        if n == 0:
            copies[0].wait_recv()
        else:
            copies[n].wait_recv()
        combine(me ^ (2 * rel), acc)
        for m, (ref, j) in enumerate(places[rel]):
            o = pltpu.make_async_copy(rcv.at[n, :, m * half:(m + 1) * half], ref.at[j], osem.at[base + 2 * n + m])
            o.start()
            outs.append(o)
    for o in outs:
        o.wait()
    for c in copies:
        c.wait_send()


class _Acc:
    def __init__(self, ref):
        self.ref = ref

    def __setitem__(self, idx, v):
        self.ref[idx] = self.ref[idx] + v


def backward_kernel(dy_hbm, x_hbm, p_ref, p48_ref, wt_ref, wloc_ref, wrt_ref, Y_hbm, h_hbm, wgu_hbm, wd_hbm,
                    sA, sB, kA, kB, Q_hbm, DH_hbm, gwr_out, gbr_out, rdx_out,
                    dyall, xall, Q, Y, PQ, h, DH, DHS, wgu, wd, snd, rcv, perm, rloc, rall, dl,
                    lsem, wsem, hsem, osem, cs, cr, rs, rr):
    me = lax.axis_index('ep')
    chip = me // 2
    in_dy = pltpu.make_async_copy(dy_hbm, dyall, lsem.at[0])
    in_y = pltpu.make_async_copy(Y_hbm, Y, lsem.at[1])
    in_x = pltpu.make_async_copy(x_hbm, xall, lsem.at[2])
    in_dy.start()
    in_y.start()

    def fetch(e):
        s = e % 2
        return (pltpu.make_async_copy(wd_hbm.at[e], wd.at[s], wsem.at[s]),
                pltpu.make_async_copy(h_hbm.at[e], h.at[s], wsem.at[2 + s]),
                pltpu.make_async_copy(wgu_hbm.at[e], wgu.at[s], wsem.at[4 + s]))

    for e in range(2):
        for c in fetch(e):
            c.start()
    in_x.start()
    entry_barrier([me ^ m for m in range(1, 8)])
    perm[...] = deinterleave_matrix()
    PQ[...] = jnp.zeros_like(PQ)
    rloc[...] = jnp.zeros_like(rloc)
    in_dy.wait()
    in_y.wait()

    def gather(q, _):
        rows_w = []
        hots = []
        racc = [jnp.zeros((R2, 1), F32) for _ in range(NE)]
        for i in range(NE):
            hot = p_ref[q, i * R2:(i + 1) * R2, :].astype(F32)
            hots.append(hot)
            rows_w.append(jnp.sum(hot * wloc_ref[q, i:i + 1, :], axis=1, keepdims=True))
        where = pl.ds(pl.multiple_of(q * R2, R2), R2)
        for nb in range(3):
            cols = slice(nb * 512, nb * 512 + 512)
            rows = dot_nn(p_ref[q], dyall[q, :, cols])
            for i in range(NE):
                r = rows[i * R2:(i + 1) * R2]
                Q[i, where, cols] = (rows_w[i] * r).astype(BF)
                racc[i] = racc[i] + jnp.sum(r * Y[i, where, cols].astype(F32), axis=1, keepdims=True)
        for i in range(NE):
            rloc[q, i:i + 1, :] = jnp.sum(hots[i] * racc[i], axis=0, keepdims=True)
        return 0

    lax.fori_loop(0, CH, gather, 0)
    rsend = [remote(rloc, rall.at[me], rs.at[m - 1], rr.at[m - 1], me ^ m) for m in range(1, 8)]
    half = D // 2
    for e in range(NE):
        s = e % 2
        cd, ch, cg = fetch(e)
        cd.wait()
        ch.wait()

        def act_grad(b, _):
            rows = pl.ds(pl.multiple_of(b * 128, 128), 128)
            gc = pl.ds(pl.multiple_of(b * 256, 256), 128)
            uc = pl.ds(pl.multiple_of(b * 256 + 128, 128), 128)
            da = dot_nt(Q[e], wd[s, rows, :])
            hg = h[s, :, gc]
            hu = h[s, :, uc]
            g = jnp.minimum(hg, LIMIT)
            u = jnp.clip(hu, -LIMIT, LIMIT)
            sg = jax.nn.sigmoid(ALPHA * g)
            gs = g * sg
            mg = jnp.where(hg < LIMIT, 1.0, jnp.where(hg == LIMIT, 0.5, 0.0))
            au = jnp.abs(hu)
            mu = jnp.where(au < LIMIT, 1.0, jnp.where(au == LIMIT, 0.5, 0.0))
            dg = da * (u + 1.0) * (sg + ALPHA * gs * (1.0 - sg)) * mg
            du = da * gs * mu
            blk = pl.ds(pl.multiple_of(b * 256, 256), 256)
            both = jnp.concatenate([dg.astype(BF), du.astype(BF)], axis=1)
            DH[e, :, blk] = dot_nt(both, perm[...]).astype(BF)
            return 0

        lax.fori_loop(0, 4, act_grad, 0)
        cg.wait()

        def p_rows(b, _):
            rows = pl.ds(pl.multiple_of(b * 512, 512), 512)
            p = dot_nt(DH[e], wgu[s, rows, :])
            for q in range(2 * CH):
                PQ[q, e * SP:e * SP + SL, rows] = p[q * SL:(q + 1) * SL].astype(BF)
            return 0

        lax.fori_loop(0, 3, p_rows, 0)
        if e + 2 < NE:
            for c in fetch(e + 2):
                c.start()
        if e == 0:
            for c in rsend:
                c.start()
            rall[me] = rloc[...]
            out_Q = pltpu.make_async_copy(Q, Q_hbm, osem.at[0])
            out_Q.start()
    out_D = pltpu.make_async_copy(DH, DH_hbm, osem.at[1])
    out_D.start()

    def combine(dev, dst):
        for nb in range(3):
            cols = slice(nb * 512, nb * 512 + 512)
            dst[:, cols] = dot_tn(p48_ref[dev], PQ[dev, :, cols])

    exchange(me, combine, snd, rcv, cs, cr, sA, sB, kA, kB, osem, 2)

    for c in rsend:
        c.wait()
    in_x.wait()
    acc = jnp.zeros((EX, D), F32)
    accb = jnp.zeros((EX, 1), F32)
    for q in range(CH):
        for k in range(2):
            lanes = slice(k * TD, (k + 1) * TD)
            w = wt_ref[2 * q + k]
            r = jnp.concatenate([rall[dv, q, 0:NE, lanes] for dv in range(2 * CH)], axis=0)
            t = w * (r - jnp.sum(w * r, axis=0, keepdims=True))
            dl[2 * q + k] = t.astype(BF)
            accb = accb + jnp.sum(t.astype(BF).astype(F32), axis=1, keepdims=True)
            acc = acc + dot_nn(dl[2 * q + k], xall[q, k * TD:(k + 1) * TD, :])
    gwr_out[...] = acc
    gbr_out[...] = jnp.broadcast_to(accb, (EX, 128))
    rdx_out[...] = dot_tn(dl[me], wrt_ref[...])
    out_Q.wait()
    out_D.wait()


def weight_grad_kernel(a_ref, b_ref, w_ref, s_ref):
    w_ref[0] = dot_tn(a_ref[0], b_ref[0])
    s_ref[0] = jnp.sum(b_ref[0].astype(F32), axis=0, keepdims=True)


def weight_grad(a, b, nblk):
    m, n = a.shape[2], b.shape[2]
    bn = n // nblk
    return pl.pallas_call(
        weight_grad_kernel,
        grid=(NE, nblk),
        in_specs=[pl.BlockSpec((1, RE, m), lambda e, j: (e, 0, 0)), pl.BlockSpec((1, RE, bn), lambda e, j: (e, 0, j))],
        out_specs=[pl.BlockSpec((1, m, bn), lambda e, j: (e, 0, j)), pl.BlockSpec((1, 1, bn), lambda e, j: (e, 0, j))],
        out_shape=[jax.ShapeDtypeStruct((NE, m, n), F32), jax.ShapeDtypeStruct((NE, 1, n), F32)],
        compiler_params=pltpu.CompilerParams(vmem_limit_bytes=32 << 20),
        cost_estimate=pl.CostEstimate(flops=2 * NE * RE * m * n, bytes_accessed=4 * NE * m * n, transcendentals=0),
    )(a, b)


def sds(shape, dt):
    return jax.ShapeDtypeStruct(shape, dt)


def solution(mesh):
    perm_of = lambda m: [(i, i ^ m) for i in range(8)]
    hop_x, hop_y = perm_of(2), perm_of(4)
    half = D // 2
    DMA = pltpu.SemaphoreType.DMA
    part_shapes = [sds((2, TD, half), F32)] * 4

    def finish(sA, sB, kA, kB, extra=None):
        a1 = lax.ppermute(sA, 'ep', hop_x)
        b1 = lax.ppermute(sB, 'ep', hop_y)
        ta, tb = kA + a1, kB + b1
        a2 = lax.ppermute(ta[1], 'ep', hop_y)
        b2 = lax.ppermute(tb[1], 'ep', hop_x)
        full = jnp.concatenate([ta[0] + a2, tb[0] + b2], axis=1)
        if extra is not None:
            full = full + extra
        return full.astype(BF)

    def local_block(hidden, grad_out, w_router, b_router, expert_ids, slot_ids, w_gate_up, b_gate_up, w_down, b_down):
        meta = jnp.concatenate([expert_ids.T, slot_ids.T], axis=0)
        wrt = w_router.T
        br = b_router[:, None]
        bgu = b_gate_up.reshape(NE, 4, 128, 2).swapaxes(2, 3).reshape(NE, 1, 2 * F)
        bd = b_down[:, None, :]
        fw = pl.pallas_call(
            forward_kernel,
            in_specs=[ANY, ANY, ANY, VM, VM, VM, VM, ANY, ANY],
            out_specs=[ANY] * 10 + [VM] * 4,
            out_shape=part_shapes + [
                sds((CH, 2 * TD, D), BF), sds((CH, 2 * TD, D), BF), sds((NE, RE, D), BF), sds((NE, RE, 2 * F), F32),
                sds((NE, RE, F), BF), sds((NE, RE, D), BF),
                sds((CH, NE * R2, 2 * TD), BF), sds((2 * CH, KC, TD), BF), sds((2 * CH, EX, TD), F32), sds((CH, 8, 2 * TD), F32)],
            scratch_shapes=[
                pltpu.VMEM((CH, 2 * TD, D), BF), pltpu.VMEM((CH, 2 * TD, D), BF), pltpu.VMEM((2 * CH, 2 * TK, TD), jnp.int32),
                pltpu.VMEM((NE, D, 2 * F), BF), pltpu.VMEM((NE, F, D), BF), pltpu.VMEM((NE, RE, D), BF), pltpu.VMEM((2, RE, D), BF),
                pltpu.VMEM((2 * CH, KC, D), BF), pltpu.VMEM((2, RE, 2 * F), F32), pltpu.VMEM((NE, RE, F), BF),
                pltpu.VMEM((2 * CH, KC, 3 * TD), BF), pltpu.VMEM((CH, TD, D), F32), pltpu.VMEM((CH, TD, D), F32),
                pltpu.VMEM((256, 256), BF),
                DMA((3,)), DMA((2 * NE,)), DMA((16,)), DMA((10,)), DMA((10,)), DMA((10,)), DMA((10,)), DMA((7,)), DMA((7,)),
                DMA((CH,)), DMA((CH,))],
            compiler_params=pltpu.CompilerParams(collective_id=0, has_side_effects=True, vmem_limit_bytes=VLIMIT),
            cost_estimate=pl.CostEstimate(flops=30_000_000_000, bytes_accessed=60_000_000, transcendentals=0),
        )(hidden, grad_out, meta, wrt, br, bgu, bd, w_gate_up, w_down)
        oA, oB, okA, okB, xall, dyall, X, h, A, Y, pm, p48, wt, wloc = fw
        block_out = finish(oA, oB, okA, okB)
        bw = pl.pallas_call(
            backward_kernel,
            in_specs=[ANY, ANY, VM, VM, VM, VM, VM, ANY, ANY, ANY, ANY],
            out_specs=[ANY] * 6 + [VM] * 3,
            out_shape=part_shapes + [sds((NE, RE, D), BF), sds((NE, RE, 2 * F), BF), sds((EX, D), F32), sds((EX, 128), F32), sds((TD, D), F32)],
            scratch_shapes=[
                pltpu.VMEM((CH, 2 * TD, D), BF), pltpu.VMEM((CH, 2 * TD, D), BF), pltpu.VMEM((NE, RE, D), BF), pltpu.VMEM((NE, RE, D), BF),
                pltpu.VMEM((2 * CH, KC, D), BF), pltpu.VMEM((2, RE, 2 * F), F32), pltpu.VMEM((NE, RE, 2 * F), BF), pltpu.VMEM((8, 128), BF),
                pltpu.VMEM((2, D, 2 * F), BF), pltpu.VMEM((2, F, D), BF), pltpu.VMEM((CH, TD, D), F32), pltpu.VMEM((CH, TD, D), F32),
                pltpu.VMEM((256, 256), BF), pltpu.VMEM((CH, 8, 2 * TD), F32), pltpu.VMEM((2 * CH, CH, 8, 2 * TD), F32),
                pltpu.VMEM((2 * CH, EX, TD), BF),
                DMA((3,)), DMA((6,)), DMA((2,)), DMA((10,)), DMA((CH,)), DMA((CH,)), DMA((7,)), DMA((7,))],
            compiler_params=pltpu.CompilerParams(collective_id=1, has_side_effects=True, vmem_limit_bytes=VLIMIT),
            cost_estimate=pl.CostEstimate(flops=30_000_000_000, bytes_accessed=60_000_000, transcendentals=0),
        )(dyall, xall, pm, p48, wt, wloc, wrt, Y, h, w_gate_up, w_down)
        dA, dB, dkA, dkB, Q, DH, gwr, gbr, rdx = bw
        grad_hidden = finish(dA, dB, dkA, dkB, rdx)
        gwgu, gbgu = weight_grad(X, DH, 4)
        gwd, gbd = weight_grad(A, Q, 3)
        return (block_out, grad_hidden, gwr.T, gbr[:, 0], gwgu, gbgu[:, 0], gwd, gbd[:, 0])

    tok_spec = P('ep', None)
    in_specs = (tok_spec, tok_spec, P(None, None), P(None), tok_spec, tok_spec, P('ep', None, None), P('ep', None), P('ep', None, None), P('ep', None))
    out_specs = (tok_spec, tok_spec, P(None, None), P(None), P('ep', None, None), P('ep', None), P('ep', None, None), P('ep', None))
    return jax.shard_map(local_block, mesh=mesh, in_specs=in_specs, out_specs=out_specs, check_vma=False)
```

```python
import functools

import jax
import jax.numpy as jnp
from jax import lax
from jax.experimental import pallas as pl
from jax.experimental.pallas import tpu as pltpu
from jax.sharding import PartitionSpec as P

LIMIT = 7.0
ALPHA = 1.702

CH = 4
EX = 40
NE = 5
TD = 128
D = 1536
F = 512
SL = 40
R2 = 2 * SL
HALF = D // 2
RE = CH * R2
SP = 48
KC = NE * SP
TK = 8
THIRDS = [slice(i, i + 512) for i in range(0, D, 512)]
BF = jnp.bfloat16
F32 = jnp.float32
ANY = pl.BlockSpec(memory_space=pl.ANY)
VM = pl.BlockSpec(memory_space=pltpu.VMEM)
VLIMIT = 67000000


def dot_nn(a, b):
    return lax.dot_general(a, b, (((1,), (0,)), ((), ())), preferred_element_type=F32)


def dot_nt(a, b):
    return lax.dot_general(a, b, (((1,), (1,)), ((), ())), preferred_element_type=F32)


def dot_tn(a, b):
    return lax.dot_general(a, b, (((0,), (0,)), ((), ())), preferred_element_type=F32)


def deinterleave_matrix():
    row = lax.broadcasted_iota(jnp.int32, (256, 256), 0)
    col = lax.broadcasted_iota(jnp.int32, (256, 256), 1)
    src = jnp.where(col < 128, 2 * col, 2 * col - 255)
    return jnp.where(row == src, 1.0, 0.0).astype(BF)


def entry_barrier(peers):
    barrier = pltpu.get_barrier_semaphore()
    for p in peers:
        pl.semaphore_signal(barrier, inc=1, device_id=(p,), device_id_type=pl.DeviceIdType.MESH)
    pl.semaphore_wait(barrier, len(peers))


def remote(src, dst, ssem, rsem, dev):
    return pltpu.make_async_remote_copy(src_ref=src, dst_ref=dst, send_sem=ssem, recv_sem=rsem,
                                        device_id=(dev,), device_id_type=pl.DeviceIdType.MESH)


class Gather:
    def __init__(self, me, own, buf, ssem, rsem):
        self.me, self.own, self.buf, self.ssem, self.rsem = me, own, buf, ssem, rsem

    def block(self, dev, lo=0, n=TD):
        core = lax.rem(dev, 2)
        return self.buf.at[dev // 2, pl.ds(pl.multiple_of(core * TD + lo, 64), n), :]

    def copy(self, slot, src, dst, dev):
        return remote(src, dst, self.ssem.at[slot], self.rsem.at[slot], dev)

    def descs(self):
        me = self.me
        c, x, y = me ^ 1, me ^ 2, me ^ 4
        own, blk, cp = self.own, self.block, self.copy
        self.x0 = cp(0, own.at[pl.ds(0, 64), :], blk(me, 0, 64), x)
        self.x1 = cp(1, own.at[pl.ds(64, 64), :], blk(me, 64, 64), x)
        self.y0 = cp(2, own.at[pl.ds(0, 64), :], blk(me, 0, 64), y)
        self.y1 = cp(3, own.at[pl.ds(64, 64), :], blk(me, 64, 64), y)
        self.d0 = cp(4, blk(x, 0, 64), blk(x, 0, 64), y)
        self.d1 = cp(5, blk(y, 64, 64), blk(y, 64, 64), x)
        self.c0 = cp(6, own, blk(me), c)
        self.c1 = cp(7, blk(x), blk(x), c)
        self.c2 = cp(8, blk(y), blk(y), c)
        self.c3 = cp(9, blk(me ^ 6), blk(me ^ 6), c)

    def start_own(self):
        self.descs()
        self.x0.start()
        self.y1.start()
        self.c0.start()
        self.x1.start()
        self.y0.start()

    def relay(self):
        self.x0.wait_recv()
        self.d0.start()
        self.y1.wait_recv()
        self.d1.start()

    def pair_xy(self):
        self.x1.wait_recv()
        self.c1.start()
        self.y0.wait_recv()
        self.c2.start()

    def pair_d(self):
        self.d0.wait_recv()
        self.d1.wait_recv()
        self.c3.start()

    def drain_sends(self):
        for d in (self.x0, self.x1, self.y0, self.y1, self.d0, self.d1, self.c0, self.c1, self.c2, self.c3):
            d.wait_send()


def split3(v):
    hi = v.astype(BF)
    r1 = v - hi.astype(F32)
    mid = r1.astype(BF)
    lo = (r1 - mid.astype(F32)).astype(BF)
    return hi, mid, lo


def block_kernel(x_hbm, dy_hbm, ids_hbm, slots_hbm, wrt_ref, br_ref, bgu_ref, bd_ref, wgu_hbm, wd_hbm,
                 sX, sY, ka0, ka1, kb0, kb1, X_hbm, A_hbm, Q_hbm, DH_hbm, h_hbm,
                 gwr_out, gbr_out, rdx_out, out_ref,
                 xall, dyall, meta, wgu, wd, XQ, YQ, h, A, DH, DHS, pw, p48, wt, wloc, bg,
                 snd, rcvo, rcvd, rab, rcv2, perm, rloc, rall, dl,
                 lsem, wsem, hsem, asem, dsem, osem, xs, xr, ds, dr, ms, mr, cs, cr, es, er, ps, pr, rs, rr, qs, qr):
    me = lax.axis_index('ep')
    chip = me // 2
    core = lax.rem(me, 2)
    mine_rows = pl.ds(pl.multiple_of(core * TD, TD), TD)
    own_m = [pltpu.make_async_copy(ids_hbm, meta.at[me, 0:TK, :], lsem.at[2]),
             pltpu.make_async_copy(slots_hbm, meta.at[me, TK:2 * TK, :], lsem.at[3])]
    own_x = pltpu.make_async_copy(x_hbm, xall.at[chip, mine_rows, :], lsem.at[0])
    own_dy = pltpu.make_async_copy(dy_hbm, dyall.at[chip, mine_rows, :], lsem.at[1])
    for c in own_m:
        c.start()
    own_x.start()
    own_dy.start()
    for e in range(NE):
        pltpu.make_async_copy(wgu_hbm.at[e], wgu.at[e], wsem.at[e]).start()
    entry_barrier([me ^ m for m in range(1, 8)])
    gx = Gather(me, x_hbm, xall, xs, xr)
    gy = Gather(me, dy_hbm, dyall, ds, dr)
    gx.start_own()
    for c in own_m:
        c.wait()
    metas = [remote(meta.at[me], meta.at[me], ms.at[m - 1], mr.at[m - 1], me ^ m) for m in range(1, 8)]
    for c in metas:
        c.start()
    for e in range(NE):
        pltpu.make_async_copy(wd_hbm.at[e], wd.at[e], wsem.at[NE + e]).start()
    perm[...] = deinterleave_matrix()
    YQ[...] = jnp.zeros_like(YQ)
    wloc[...] = jnp.zeros_like(wloc)
    rloc[...] = jnp.zeros_like(rloc)
    for b in range(4):
        cols = slice(b * 256, b * 256 + 256)
        bg[:, cols] = sum(dot_nn(part, perm[...]) for part in split3(bgu_ref[:, cols]))
    eye = lax.broadcasted_iota(jnp.int32, (EX, EX), 0) == lax.broadcasted_iota(jnp.int32, (EX, EX), 1)
    br_col = jnp.sum(jnp.where(eye, br_ref[...], 0.0), axis=1, keepdims=True)

    def permute(e):
        pltpu.make_async_copy(wgu_hbm.at[e], wgu.at[e], wsem.at[e]).wait()

        def body(b, _):
            cols = pl.ds(pl.multiple_of(b * 256, 256), 256)
            for r in range(3):
                rows = slice(r * 512, r * 512 + 512)
                wgu[e, rows, cols] = dot_nn(wgu[e, rows, cols], perm[...]).astype(BF)
            return 0

        lax.fori_loop(0, 4, body, 0)

    permute(0)
    permute(1)
    gx.relay()
    gy.start_own()
    permute(2)
    permute(3)
    own_x.wait()
    for c in metas:
        c.wait()
    permute(4)

    iota40 = lax.broadcasted_iota(jnp.int32, (EX, TD), 0)
    iota48 = lax.broadcasted_iota(jnp.int32, (SP, TD), 0)

    def route(q):
        lt = dot_nt(wrt_ref[...], xall[q]) + br_col
        for k in range(2):
            ids = meta[2 * q + k, 0:TK, :]
            slt = meta[2 * q + k, TK:2 * TK, :]
            slot = jnp.full((EX, TD), -1, jnp.int32)
            chosen = jnp.zeros((EX, TD), jnp.int32)
            for j in range(TK):
                hit = ids[j:j + 1, :] == iota40
                slot = jnp.where(hit, slt[j:j + 1, :], slot)
                chosen = jnp.where(hit, 1, chosen)
            on = chosen == 1
            lk = lt[:, k * TD:(k + 1) * TD]
            mx = jnp.max(jnp.where(on, lk, -jnp.inf), axis=0, keepdims=True)
            ex = jnp.where(on, jnp.exp(lk - mx), 0.0)
            w = ex / jnp.sum(ex, axis=0, keepdims=True)
            wt[2 * q + k] = w
            slotf = slot.astype(F32)
            for i in range(NE):
                mine = iota40 == me * NE + i
                s = jnp.max(jnp.where(mine, slotf, -1.0), axis=0, keepdims=True)
                wv = jnp.sum(jnp.where(mine, w, 0.0), axis=0, keepdims=True)
                hot = s.astype(jnp.int32) == iota48
                p48[2 * q + k, i * SP:(i + 1) * SP, :] = jnp.where(hot, 1.0, 0.0).astype(BF)
                for n, part in enumerate(split3(jnp.where(hot, wv, 0.0))):
                    pw[2 * q + k, i * SP:(i + 1) * SP, n * TD:(n + 1) * TD] = part
                wloc[2 * q + k, i:i + 1, :] = wv
        where = pl.ds(pl.multiple_of(q * R2, R2), R2)
        for nb in range(3):
            cols = slice(nb * 512, nb * 512 + 512)
            rows = [dot_nn(p48[2 * q + k], xall[q, k * TD:(k + 1) * TD, cols]) for k in range(2)]
            for i in range(NE):
                XQ[i, where, cols] = jnp.concatenate([r[i * SP:i * SP + SL] for r in rows], axis=0).astype(BF)

    gx.c0.wait_recv()
    route(chip)
    gx.pair_xy()
    gx.pair_d()
    gx.c1.wait_recv()
    gx.c2.wait_recv()

    def route_next(i, _):
        route(chip ^ i)
        return 0

    lax.fori_loop(1, 3, route_next, 0)
    gx.c3.wait_recv()
    route(chip ^ 3)
    out_X = pltpu.make_async_copy(XQ, X_hbm, osem.at[0])
    out_X.start()

    def h_out(e):
        return pltpu.make_async_copy(h.at[lax.rem(e, 2)], h_hbm.at[e], hsem.at[lax.rem(e, 2)])

    def h_in(e):
        return pltpu.make_async_copy(h_hbm.at[e], h.at[lax.rem(e, 2)], hsem.at[2 + lax.rem(e, 2)])

    def a_out(e):
        return pltpu.make_async_copy(A.at[lax.rem(e, 2)], A_hbm.at[e], asem.at[lax.rem(e, 2)])

    def expert(e, _):
        slot = lax.rem(e, 2)

        @pl.when(e >= 2)
        def _():
            h_out(e - 2).wait()
            a_out(e - 2).wait()

        for b in range(4):
            cols = slice(b * 256, b * 256 + 256)
            pre = dot_nn(XQ[e], wgu[e, :, cols]) + bg[pl.ds(e, 1), cols]
            hg, hu = pre[:, :128], pre[:, 128:]
            g = jnp.minimum(hg, LIMIT)
            u1 = jnp.clip(hu, -LIMIT, LIMIT) + 1.0
            sg = jax.nn.sigmoid(ALPHA * g)
            gs = g * sg
            A[slot, :, b * 128:b * 128 + 128] = (gs * u1).astype(BF)
            au = jnp.abs(hu)
            mg = jnp.where(hg < LIMIT, 1.0, jnp.where(hg == LIMIT, 0.5, 0.0))
            mu = jnp.where(au < LIMIT, 1.0, jnp.where(au == LIMIT, 0.5, 0.0))
            h[slot, :, b * 256:b * 256 + 128] = u1 * (sg + ALPHA * gs * (1.0 - sg)) * mg
            h[slot, :, b * 256 + 128:b * 256 + 256] = gs * mu
        a_out(e).start()

        @pl.when(e < 3)
        def _():
            h_out(e).start()

        pltpu.make_async_copy(wd_hbm.at[e], wd.at[e], wsem.at[NE + e]).wait()
        yrow = pl.ds(pl.multiple_of(e * SP, SP), SL)
        for b in range(3):
            cols = slice(b * 512, b * 512 + 512)
            y = dot_nn(A[slot], wd[e, :, cols]) + bd_ref[pl.ds(e, 1), cols]
            for q in range(2 * CH):
                YQ[q, yrow, cols] = y[q * SL:(q + 1) * SL].astype(BF)

        @pl.when(e == 0)
        def _():
            gy.relay()

        @pl.when(e == 2)
        def _():
            gy.pair_xy()

        return 0

    lax.fori_loop(0, NE, expert, 0)

    def combine_y(dev, cols):
        full = dot_tn(pw[dev], YQ[dev, :, cols])
        return full[0:TD] + full[TD:2 * TD] + full[2 * TD:3 * TD]

    first = [remote(rcvo.at[0, :, 0:HALF], rab.at[0, 1], ps.at[0], pr.at[0], me ^ 2),
             remote(rcvo.at[0, :, HALF:D], rab.at[1, 1], ps.at[1], pr.at[1], me ^ 4),
             remote(rcvo.at[1, :, 0:HALF], rab.at[0, 0], ps.at[2], pr.at[2], me ^ 2),
             remote(rcvo.at[2, :, HALF:D], rab.at[1, 0], ps.at[3], pr.at[3], me ^ 4)]

    ycopies = pair_copies(me, snd, rcvo, cs, cr)
    send_blocks(me, combine_y, snd, ycopies)
    ycopies[CH - 1].start()
    add_block(me, combine_y, rcvo, ycopies, 0)
    add_block(me, combine_y, rcvo, ycopies, 1)
    first[0].start()
    first[1].start()
    add_block(me, combine_y, rcvo, ycopies, 2)
    first[2].start()
    gy.pair_d()
    add_block(me, combine_y, rcvo, ycopies, 3)
    first[3].start()

    gy.c0.wait_recv()
    gy.c1.wait_recv()
    gy.c2.wait_recv()
    gy.c3.wait_recv()
    own_dy.wait()
    out_X.wait()

    def gather(q, _):
        weights, hots, racc = [], [], []
        for k in range(2):
            hot = p48[2 * q + k].astype(F32)
            hots.append(hot)
            weights.append([jnp.sum(hot[i * SP:(i + 1) * SP] * wloc[2 * q + k, i:i + 1, :], axis=1, keepdims=True)
                            for i in range(NE)])
            racc.append(jnp.zeros((KC, 1), F32))
        where = pl.ds(pl.multiple_of(q * R2, R2), R2)
        for nb in range(3):
            cols = slice(nb * 512, nb * 512 + 512)
            rows = [dot_nn(p48[2 * q + k], dyall[q, k * TD:(k + 1) * TD, cols]) for k in range(2)]
            for i in range(NE):
                XQ[i, where, cols] = jnp.concatenate(
                    [weights[k][i][0:SL] * rows[k][i * SP:i * SP + SL] for k in range(2)], axis=0).astype(BF)
            for k in range(2):
                racc[k] = racc[k] + jnp.sum(rows[k] * YQ[2 * q + k, :, cols].astype(F32), axis=1, keepdims=True)
        for k in range(2):
            rh = hots[k] * racc[k]
            for i in range(NE):
                rloc[2 * q + k, i:i + 1, :] = jnp.sum(rh[i * SP:(i + 1) * SP], axis=0, keepdims=True)
        return 0

    lax.fori_loop(0, CH, gather, 0)
    for e in (3, 4):
        a_out(e).wait()
    for c in ycopies:
        c.wait_send()
    rsend = [remote(rloc, rall.at[me], rs.at[m - 1], rr.at[m - 1], me ^ m) for m in range(1, 8)]
    out_Q = pltpu.make_async_copy(XQ, Q_hbm, osem.at[1])
    out_Q.start()

    def d_out(n):
        return pltpu.make_async_copy(DH.at[lax.rem(n, 2)], DH_hbm.at[NE - 1 - n], dsem.at[lax.rem(n, 2)])

    second = [remote(rab.at[0, 1], rcv2.at[0], qs.at[0], qr.at[0], me ^ 4),
              remote(rab.at[1, 1], rcv2.at[1], qs.at[1], qr.at[1], me ^ 2)]

    def expert_back(n, _):
        e = NE - 1 - n
        slot = lax.rem(e, 2)
        dslot = lax.rem(n, 2)

        @pl.when(n >= 2)
        def _():
            h_in(e).wait()
            d_out(n - 2).wait()

        da = dot_nt(XQ[e], wd[e])
        for b in range(4):
            lo = b * 256
            d = da[:, b * 128:b * 128 + 128]
            DHS[:, lo:lo + 128] = (d * h[slot, :, lo:lo + 128]).astype(BF)
            DHS[:, lo + 128:lo + 256] = (d * h[slot, :, lo + 128:lo + 256]).astype(BF)

        @pl.when(n < 3)
        def _():
            h_in(e - 2).start()

        prow = pl.ds(pl.multiple_of(e * SP, SP), SL)
        for b in range(3):
            cols = slice(b * 512, b * 512 + 512)
            p = dot_nt(DHS[...], wgu[e, cols, :])
            for q in range(2 * CH):
                YQ[q, prow, cols] = p[q * SL:(q + 1) * SL].astype(BF)
        for b in range(4):
            cols = slice(b * 256, b * 256 + 256)
            DH[dslot, :, cols] = dot_nt(DHS[:, cols], perm[...]).astype(BF)
        d_out(n).start()

        @pl.when(n == 0)
        def _():
            for c in rsend:
                c.start()

        @pl.when(n == 2)
        def _():
            for m in range(2):
                first[m].wait_recv()
                rab[m, 1] = rab[m, 1] + rcvo[2 - m, :, m * HALF:(m + 1) * HALF]

        @pl.when(n == 3)
        def _():
            for c in second:
                c.start()

        return 0

    lax.fori_loop(0, NE, expert_back, 0)
    rall[me] = rloc[...]
    d_out(3).wait()
    d_out(4).wait()

    def combine_p(dev, cols):
        return dot_tn(p48[dev], YQ[dev, :, cols])

    pcopies = pair_copies(me, snd, rcvd, es, er)
    send_blocks(me, combine_p, snd, pcopies)
    outs = []
    places = ((sX.at[1], sY.at[1]), (sX.at[0], kb1), (ka1, sY.at[0]), (ka0, kb0))

    def finish_p(n):
        add_block(me, combine_p, rcvd, pcopies, n)
        for m, dst in enumerate(places[n]):
            o = pltpu.make_async_copy(rcvd.at[n, :, m * HALF:(m + 1) * HALF], dst, osem.at[2 + 2 * n + m])
            o.start()
            outs.append(o)

    for c in rsend:
        c.wait()
    pcopies[CH - 1].start()
    acc = jnp.zeros((EX, D), F32)
    accb = jnp.zeros((EX, 1), F32)
    for v in range(2 * CH):
        w = wt[v]
        r = jnp.concatenate([rall[dv, v, 0:NE, :] for dv in range(2 * CH)], axis=0)
        t = w * (r - jnp.sum(w * r, axis=0, keepdims=True))
        dl[v] = t.astype(BF)
        accb = accb + jnp.sum(t.astype(BF).astype(F32), axis=1, keepdims=True)
        acc = acc + dot_nn(dl[v], xall[v // 2, (v % 2) * TD:(v % 2) * TD + TD, :])
    gwr_out[...] = acc
    gbr_out[...] = jnp.broadcast_to(accb, (EX, 128))
    rdx_out[...] = dot_tn(dl[me], wrt_ref[...])

    for n in range(CH):
        finish_p(n)
    for n in range(2):
        first[2 + n].wait_recv()
        second[n].wait()
        lanes = slice(n * HALF, n * HALF + HALF)
        out_ref[:, lanes] = (rab[n, 0] + rcvo[3, :, lanes] + rcv2[n]).astype(BF)
    for o in outs:
        o.wait()
    for c in pcopies:
        c.wait_send()
    out_Q.wait()
    for c in first:
        c.wait_send()
    gx.drain_sends()
    gy.drain_sends()


ORDER = (3, 1, 2, 0)


def pair_copies(me, snd, rcv, cs, cr):
    return [remote(snd.at[n], rcv.at[n], cs.at[n], cr.at[n], me ^ 1) for n in range(CH)]


def send_blocks(me, combine, snd, copies):
    for n, rel in enumerate(ORDER):
        for cols in THIRDS:
            snd[n, :, cols] = combine(me ^ 1 ^ (2 * rel), cols)
        if n:
            copies[n - 1].start()


def add_block(me, combine, rcv, copies, n):
    vals = [combine(me ^ (2 * ORDER[n]), cols) for cols in THIRDS]
    copies[n].wait_recv()
    for cols, v in zip(THIRDS, vals):
        rcv[n, :, cols] = rcv[n, :, cols] + v


def resident_kernel(a_ref, b_ref, w_ref, s_ref):
    e, j = pl.program_id(0), pl.program_id(1)
    bm = w_ref.shape[1]

    @pl.when(j == 0)
    def _():
        s_ref[pl.ds(e, 1), :] = jnp.sum(b_ref[e].astype(F32), axis=0, keepdims=True)

    w_ref[0] = dot_tn(a_ref[e, :, pl.ds(pl.multiple_of(j * bm, bm), bm)], b_ref[e])


def weight_grad_kernel(a_hbm, b_hbm, w_ref, s_ref, a_v, b_v, sem):
    e, j = pl.program_id(0), pl.program_id(1)
    bm = w_ref.shape[1]

    def fetch(n):
        return (pltpu.make_async_copy(a_hbm.at[n], a_v.at[n], sem.at[0, n]),
                pltpu.make_async_copy(b_hbm.at[n], b_v.at[n], sem.at[1, n]))

    @pl.when((e == 0) & (j == 0))
    def _():
        for n in range(NE):
            for c in fetch(n):
                c.start()

    @pl.when(j == 0)
    def _():
        for c in fetch(e):
            c.wait()
        s_ref[pl.ds(e, 1), :] = jnp.sum(b_v[e].astype(F32), axis=0, keepdims=True)

    w_ref[0] = dot_tn(a_v[e, :, pl.ds(pl.multiple_of(j * bm, bm), bm)], b_v[e])


def weight_grad(a, b, nblk, resident):
    m, n = a.shape[2], b.shape[2]
    bm = m // nblk
    return pl.pallas_call(
        resident_kernel if resident else weight_grad_kernel,
        grid=(NE, nblk),
        in_specs=[VM if resident else pl.BlockSpec(memory_space=pltpu.HBM)] * 2,
        out_specs=[pl.BlockSpec((1, bm, n), lambda e, j: (e, j, 0)), pl.BlockSpec((NE, n), lambda e, j: (0, 0))],
        out_shape=[jax.ShapeDtypeStruct((NE, m, n), F32), jax.ShapeDtypeStruct((NE, n), F32)],
        scratch_shapes=[] if resident else [pltpu.VMEM(a.shape, BF), pltpu.VMEM(b.shape, BF), pltpu.SemaphoreType.DMA((2, NE))],
        compiler_params=pltpu.CompilerParams(vmem_limit_bytes=60 << 20),
        cost_estimate=pl.CostEstimate(flops=2 * NE * RE * m * n, bytes_accessed=4 * NE * m * n, transcendentals=0),
    )(a, b)


def sds(shape, dt):
    return jax.ShapeDtypeStruct(shape, dt)


def solution(mesh):
    perm_of = lambda m: [(i, i ^ m) for i in range(8)]
    hop_x, hop_y = perm_of(2), perm_of(4)
    DMA = pltpu.SemaphoreType.DMA
    part = sds((TD, HALF), F32)
    hops = sds((2, TD, HALF), F32)

    def local_block(hidden, grad_out, w_router, b_router, expert_ids, slot_ids, w_gate_up, b_gate_up, w_down, b_down):
        wrt = w_router.T
        outs = pl.pallas_call(
            block_kernel,
            in_specs=[ANY, ANY, ANY, ANY, VM, VM, VM, VM, ANY, ANY],
            out_specs=[ANY] * 11 + [VM] * 4,
            out_shape=[hops] * 2 + [part] * 4 + [
                sds((NE, RE, D), BF), sds((NE, RE, F), BF), sds((NE, RE, D), BF), sds((NE, RE, 2 * F), BF), sds((3, RE, 2 * F), F32),
                sds((EX, D), F32), sds((EX, 128), F32), sds((TD, D), F32), sds((TD, D), BF)],
            scratch_shapes=[
                pltpu.VMEM((CH, 2 * TD, D), BF), pltpu.VMEM((CH, 2 * TD, D), BF), pltpu.VMEM((2 * CH, 2 * TK, TD), jnp.int32),
                pltpu.VMEM((NE, D, 2 * F), BF), pltpu.VMEM((NE, F, D), BF), pltpu.VMEM((NE, RE, D), BF), pltpu.VMEM((2 * CH, KC, D), BF),
                pltpu.VMEM((2, RE, 2 * F), F32), pltpu.VMEM((2, RE, F), BF), pltpu.VMEM((2, RE, 2 * F), BF), pltpu.VMEM((RE, 2 * F), BF),
                pltpu.VMEM((2 * CH, KC, 3 * TD), BF), pltpu.VMEM((2 * CH, KC, TD), BF), pltpu.VMEM((2 * CH, EX, TD), F32),
                pltpu.VMEM((2 * CH, 8, TD), F32), pltpu.VMEM((NE, 2 * F), F32),
                pltpu.VMEM((CH, TD, D), F32), pltpu.VMEM((CH, TD, D), F32), pltpu.VMEM((CH, TD, D), F32),
                pltpu.VMEM((2, 2, TD, HALF), F32), pltpu.VMEM((2, TD, HALF), F32), pltpu.VMEM((256, 256), BF),
                pltpu.VMEM((2 * CH, 8, TD), F32), pltpu.VMEM((2 * CH, 2 * CH, 8, TD), F32), pltpu.VMEM((2 * CH, EX, TD), BF),
                DMA((4,)), DMA((2 * NE,)), DMA((4,)), DMA((2,)), DMA((2,)), DMA((10,)),
                *[DMA((10,))] * 4, *[DMA((7,))] * 2,
                *[DMA((CH,))] * 6, *[DMA((7,))] * 2, *[DMA((2,))] * 2],
            compiler_params=pltpu.CompilerParams(collective_id=0, has_side_effects=True, vmem_limit_bytes=VLIMIT),
            cost_estimate=pl.CostEstimate(flops=50_000_000_000, bytes_accessed=60_000_000, transcendentals=0),
        )(hidden, grad_out, expert_ids.T, slot_ids.T, wrt, b_router[None, :], b_gate_up, b_down, w_gate_up, w_down)
        sX, sY, ka0, ka1, kb0, kb1, X, A, Q, DH, _, gwr, gbr, rdx, block_out = outs
        rX = lax.ppermute(sX, 'ep', hop_x)
        rY = lax.ppermute(sY, 'ep', hop_y)
        gwgu, gbgu = weight_grad(X, DH, 2, False)
        ka1, kb1, gbgu = lax.optimization_barrier((ka1, kb1, gbgu))
        ta = ka1 + rX[1]
        tb = kb1 + rY[1]
        ta, tb, A = lax.optimization_barrier((ta, tb, A))
        gwd, gbd = weight_grad(A, Q, 1, False)
        a2 = lax.ppermute(ta, 'ep', hop_y)
        b2 = lax.ppermute(tb, 'ep', hop_x)
        grad_hidden = (jnp.concatenate([ka0 + rX[0] + a2, kb0 + rY[0] + b2], axis=1) + rdx).astype(BF)
        return (block_out, grad_hidden, gwr.T, gbr[:, 0], gwgu, gbgu, gwd, gbd)

    row = P('ep')
    in_specs = (row, row, P(), P(), row, row, row, row, row, row)
    out_specs = (row, row, P(), P(), row, row, row, row)
    return jax.shard_map(local_block, mesh=mesh, in_specs=in_specs, out_specs=out_specs, check_vma=False)
```

```python
import functools

import jax
import jax.numpy as jnp
from jax import lax
from jax.experimental import pallas as pl
from jax.experimental.pallas import tpu as pltpu
from jax.sharding import PartitionSpec as P

LIMIT = 7.0
ALPHA = 1.702

CH = 4
ND = 2 * CH
PEERS = range(1, ND)
EX = 40
NE = 5
TD = 128
D = 1536
F = 512
SL = 40
R2 = 2 * SL
HALF = D // 2
RE = CH * R2
SP = 48
KC = NE * SP
TK = 8
THIRDS = [slice(i, i + 512) for i in range(0, D, 512)]
BF = jnp.bfloat16
F32 = jnp.float32
ANY = pl.BlockSpec(memory_space=pl.ANY)
VM = pl.BlockSpec(memory_space=pltpu.VMEM)
VLIMIT = 67000000


def dot_nn(a, b):
    return lax.dot_general(a, b, (((1,), (0,)), ((), ())), preferred_element_type=F32)


def dot_nt(a, b):
    return lax.dot_general(a, b, (((1,), (1,)), ((), ())), preferred_element_type=F32)


def dot_tn(a, b):
    return lax.dot_general(a, b, (((0,), (0,)), ((), ())), preferred_element_type=F32)


def deinterleave_matrix():
    row = lax.broadcasted_iota(jnp.int32, (256, 256), 0)
    col = lax.broadcasted_iota(jnp.int32, (256, 256), 1)
    src = jnp.where(col < 128, 2 * col, 2 * col - 255)
    return jnp.where(row == src, 1.0, 0.0).astype(BF)


def entry_barrier(peers):
    barrier = pltpu.get_barrier_semaphore()
    for p in peers:
        pl.semaphore_signal(barrier, inc=1, device_id=(p,), device_id_type=pl.DeviceIdType.MESH)
    pl.semaphore_wait(barrier, len(peers))


def remote(src, dst, ssem, rsem, dev):
    return pltpu.make_async_remote_copy(src_ref=src, dst_ref=dst, send_sem=ssem, recv_sem=rsem,
                                        device_id=(dev,), device_id_type=pl.DeviceIdType.MESH)


class Gather:
    def __init__(self, me, own, buf, ssem, rsem):
        self.me, self.own, self.buf, self.ssem, self.rsem = me, own, buf, ssem, rsem

    def block(self, dev, lo=0, n=TD):
        core = lax.rem(dev, 2)
        return self.buf.at[dev // 2, pl.ds(pl.multiple_of(core * TD + lo, 64), n), :]

    def copy(self, slot, src, dst, dev):
        return remote(src, dst, self.ssem.at[slot], self.rsem.at[slot], dev)

    def descs(self):
        me = self.me
        c, x, y = me ^ 1, me ^ 2, me ^ 4
        own, blk, cp = self.own, self.block, self.copy
        self.x0 = cp(0, own.at[pl.ds(0, 64), :], blk(me, 0, 64), x)
        self.x1 = cp(1, own.at[pl.ds(64, 64), :], blk(me, 64, 64), x)
        self.y0 = cp(2, own.at[pl.ds(0, 64), :], blk(me, 0, 64), y)
        self.y1 = cp(3, own.at[pl.ds(64, 64), :], blk(me, 64, 64), y)
        self.d0 = cp(4, blk(x, 0, 64), blk(x, 0, 64), y)
        self.d1 = cp(5, blk(y, 64, 64), blk(y, 64, 64), x)
        self.c0 = cp(6, own, blk(me), c)
        self.c1 = cp(7, blk(x), blk(x), c)
        self.c2 = cp(8, blk(y), blk(y), c)
        self.c3 = cp(9, blk(me ^ 6), blk(me ^ 6), c)

    def start_own(self):
        self.descs()
        self.x0.start()
        self.y1.start()
        self.c0.start()
        self.x1.start()
        self.y0.start()

    def relay(self):
        self.x0.wait_recv()
        self.d0.start()
        self.y1.wait_recv()
        self.d1.start()

    def pair_xy(self):
        self.x1.wait_recv()
        self.c1.start()
        self.y0.wait_recv()
        self.c2.start()

    def pair_d(self):
        self.d0.wait_recv()
        self.d1.wait_recv()
        self.c3.start()

    def drain_sends(self):
        for d in (self.x0, self.x1, self.y0, self.y1, self.d0, self.d1, self.c0, self.c1, self.c2, self.c3):
            d.wait_send()


def split3(v):
    hi = v.astype(BF)
    r1 = v - hi.astype(F32)
    mid = r1.astype(BF)
    lo = (r1 - mid.astype(F32)).astype(BF)
    return hi, mid, lo


def block_kernel(x_hbm, dy_hbm, ids_hbm, slots_hbm, wrt_ref, br_ref, bgu_ref, bd_ref, wgu_hbm, wd_hbm,
                 sX, sY, ka0, ka1, kb0, kb1, X_hbm, A_hbm, Q_hbm, DH_hbm, h_hbm,
                 gwr_out, gbr_out, out_ref,
                 xall, dyall, meta, wgu, wd, XQ, YQ, h, A, DH, DHS, pw, p48, wt, wloc, bg,
                 snd, rcvo, rcvd, rab, rcv2, perm, rloc, rall, dl,
                 lsem, wsem, hsem, asem, dsem, osem, xs, xr, ds, dr, ms, mr, cs, cr, es, er, ps, pr, rs, rr, qs, qr):
    me = lax.axis_index('ep')
    chip = me // 2
    core = lax.rem(me, 2)
    mine_rows = pl.ds(pl.multiple_of(core * TD, TD), TD)
    own_m = [pltpu.make_async_copy(ids_hbm, meta.at[me, 0:TK, :], lsem.at[2]),
             pltpu.make_async_copy(slots_hbm, meta.at[me, TK:2 * TK, :], lsem.at[3])]
    own_x = pltpu.make_async_copy(x_hbm, xall.at[chip, mine_rows, :], lsem.at[0])
    own_dy = pltpu.make_async_copy(dy_hbm, dyall.at[chip, mine_rows, :], lsem.at[1])
    for c in own_m:
        c.start()
    own_x.start()
    own_dy.start()
    for e in range(NE):
        pltpu.make_async_copy(wgu_hbm.at[e], wgu.at[e], wsem.at[e]).start()
    entry_barrier([me ^ m for m in PEERS])
    gx = Gather(me, x_hbm, xall, xs, xr)
    gy = Gather(me, dy_hbm, dyall, ds, dr)
    gx.start_own()
    for c in own_m:
        c.wait()
    metas = [remote(meta.at[me], meta.at[me], ms.at[m - 1], mr.at[m - 1], me ^ m) for m in PEERS]
    for c in metas:
        c.start()
    for e in range(NE):
        pltpu.make_async_copy(wd_hbm.at[e], wd.at[e], wsem.at[NE + e]).start()
    perm[...] = deinterleave_matrix()
    YQ[...] = jnp.zeros_like(YQ)
    wloc[...] = jnp.zeros_like(wloc)
    rloc[...] = jnp.zeros_like(rloc)
    for b in range(4):
        cols = slice(b * 256, b * 256 + 256)
        bg[:, cols] = sum(dot_nn(part, perm[...]) for part in split3(bgu_ref[:, cols]))
    eye = lax.broadcasted_iota(jnp.int32, (EX, EX), 0) == lax.broadcasted_iota(jnp.int32, (EX, EX), 1)
    br_col = jnp.sum(jnp.where(eye, br_ref[...], 0.0), axis=1, keepdims=True)

    def permute(e):
        pltpu.make_async_copy(wgu_hbm.at[e], wgu.at[e], wsem.at[e]).wait()

        def body(b, _):
            cols = pl.ds(pl.multiple_of(b * 256, 256), 256)
            for r in range(3):
                rows = slice(r * 512, r * 512 + 512)
                wgu[e, rows, cols] = dot_nn(wgu[e, rows, cols], perm[...]).astype(BF)
            return 0

        lax.fori_loop(0, 4, body, 0)

    permute(0)
    permute(1)
    gx.relay()
    gy.start_own()
    permute(2)
    permute(3)
    own_x.wait()
    for c in metas:
        c.wait()
    permute(4)

    iota40 = lax.broadcasted_iota(jnp.int32, (EX, TD), 0)
    iota48 = lax.broadcasted_iota(jnp.int32, (SP, TD), 0)

    def route(q):
        lt = dot_nt(wrt_ref[...], xall[q]) + br_col
        for k in range(2):
            ids = meta[2 * q + k, 0:TK, :]
            slt = meta[2 * q + k, TK:2 * TK, :]
            slot = jnp.full((EX, TD), -1, jnp.int32)
            chosen = jnp.zeros((EX, TD), jnp.int32)
            for j in range(TK):
                hit = ids[j:j + 1, :] == iota40
                slot = jnp.where(hit, slt[j:j + 1, :], slot)
                chosen = jnp.where(hit, 1, chosen)
            on = chosen == 1
            lk = lt[:, k * TD:(k + 1) * TD]
            mx = jnp.max(jnp.where(on, lk, -jnp.inf), axis=0, keepdims=True)
            ex = jnp.where(on, jnp.exp(lk - mx), 0.0)
            w = ex / jnp.sum(ex, axis=0, keepdims=True)
            wt[2 * q + k] = w
            slotf = slot.astype(F32)
            for i in range(NE):
                mine = iota40 == me * NE + i
                s = jnp.max(jnp.where(mine, slotf, -1.0), axis=0, keepdims=True)
                wv = jnp.sum(jnp.where(mine, w, 0.0), axis=0, keepdims=True)
                hot = s.astype(jnp.int32) == iota48
                p48[2 * q + k, i * SP:(i + 1) * SP, :] = jnp.where(hot, 1.0, 0.0).astype(BF)
                for n, part in enumerate(split3(jnp.where(hot, wv, 0.0))):
                    pw[2 * q + k, i * SP:(i + 1) * SP, n * TD:(n + 1) * TD] = part
                wloc[2 * q + k, i:i + 1, :] = wv
        where = pl.ds(pl.multiple_of(q * R2, R2), R2)
        for nb in range(3):
            cols = slice(nb * 512, nb * 512 + 512)
            rows = [dot_nn(p48[2 * q + k], xall[q, k * TD:(k + 1) * TD, cols]) for k in range(2)]
            for i in range(NE):
                XQ[i, where, cols] = jnp.concatenate([r[i * SP:i * SP + SL] for r in rows], axis=0).astype(BF)

    gx.c0.wait_recv()
    route(chip)
    gx.pair_xy()
    gx.pair_d()
    gx.c1.wait_recv()
    gx.c2.wait_recv()

    def route_next(i, _):
        route(chip ^ i)
        return 0

    lax.fori_loop(1, 3, route_next, 0)
    gx.c3.wait_recv()
    route(chip ^ 3)
    out_X = pltpu.make_async_copy(XQ, X_hbm, osem.at[0])
    out_X.start()

    def h_out(e):
        return pltpu.make_async_copy(h.at[lax.rem(e, 2)], h_hbm.at[e], hsem.at[lax.rem(e, 2)])

    def h_in(e):
        return pltpu.make_async_copy(h_hbm.at[e], h.at[lax.rem(e, 2)], hsem.at[2 + lax.rem(e, 2)])

    def a_out(e):
        return pltpu.make_async_copy(A.at[lax.rem(e, 2)], A_hbm.at[e], asem.at[lax.rem(e, 2)])

    def expert(e, _):
        slot = lax.rem(e, 2)

        @pl.when(e >= 2)
        def _():
            h_out(e - 2).wait()
            a_out(e - 2).wait()

        for b in range(4):
            cols = slice(b * 256, b * 256 + 256)
            pre = dot_nn(XQ[e], wgu[e, :, cols]) + bg[pl.ds(e, 1), cols]
            hg, hu = pre[:, :128], pre[:, 128:]
            g = jnp.minimum(hg, LIMIT)
            u1 = jnp.clip(hu, -LIMIT, LIMIT) + 1.0
            sg = jax.nn.sigmoid(ALPHA * g)
            gs = g * sg
            A[slot, :, b * 128:b * 128 + 128] = (gs * u1).astype(BF)
            au = jnp.abs(hu)
            mg = jnp.where(hg < LIMIT, 1.0, jnp.where(hg == LIMIT, 0.5, 0.0))
            mu = jnp.where(au < LIMIT, 1.0, jnp.where(au == LIMIT, 0.5, 0.0))
            h[slot, :, b * 256:b * 256 + 128] = u1 * (sg + ALPHA * gs * (1.0 - sg)) * mg
            h[slot, :, b * 256 + 128:b * 256 + 256] = gs * mu
        a_out(e).start()

        @pl.when(e < 3)
        def _():
            h_out(e).start()

        pltpu.make_async_copy(wd_hbm.at[e], wd.at[e], wsem.at[NE + e]).wait()
        yrow = pl.ds(pl.multiple_of(e * SP, SP), SL)
        for b in range(3):
            cols = slice(b * 512, b * 512 + 512)
            y = dot_nn(A[slot], wd[e, :, cols]) + bd_ref[pl.ds(e, 1), cols]
            for q in range(ND):
                YQ[q, yrow, cols] = y[q * SL:(q + 1) * SL].astype(BF)

        @pl.when(e == 0)
        def _():
            gy.relay()

        @pl.when(e == 2)
        def _():
            gy.pair_xy()

        return 0

    lax.fori_loop(0, NE, expert, 0)

    def combine_y(dev, cols):
        full = dot_tn(pw[dev], YQ[dev, :, cols])
        return full[0:TD] + full[TD:2 * TD] + full[2 * TD:3 * TD]

    first = [remote(rcvo.at[0, :, 0:HALF], rab.at[0, 1], ps.at[0], pr.at[0], me ^ 2),
             remote(rcvo.at[0, :, HALF:D], rab.at[1, 1], ps.at[1], pr.at[1], me ^ 4),
             remote(rcvo.at[1, :, 0:HALF], rab.at[0, 0], ps.at[2], pr.at[2], me ^ 2),
             remote(rcvo.at[2, :, HALF:D], rab.at[1, 0], ps.at[3], pr.at[3], me ^ 4)]

    ycopies = pair_copies(me, snd, rcvo, cs, cr)
    for n in range(CH - 1):
        send_block(me, combine_y, snd, ycopies, n)
    add_block(me, combine_y, rcvo, ycopies, 0)
    send_block(me, combine_y, snd, ycopies, 3)
    first[0].start()
    first[1].start()
    ycopies[CH - 1].start()
    add_block(me, combine_y, rcvo, ycopies, 1)
    add_block(me, combine_y, rcvo, ycopies, 2)
    first[2].start()
    gy.pair_d()
    add_block(me, combine_y, rcvo, ycopies, 3)
    first[3].start()

    gy.c0.wait_recv()
    gy.c1.wait_recv()
    gy.c2.wait_recv()
    gy.c3.wait_recv()
    own_dy.wait()
    out_X.wait()

    def gather(q, _):
        weights, hots, racc = [], [], []
        for k in range(2):
            hot = p48[2 * q + k].astype(F32)
            hots.append(hot)
            weights.append([jnp.sum(hot[i * SP:(i + 1) * SP] * wloc[2 * q + k, i:i + 1, :], axis=1, keepdims=True)
                            for i in range(NE)])
            racc.append(jnp.zeros((KC, 1), F32))
        where = pl.ds(pl.multiple_of(q * R2, R2), R2)
        for nb in range(3):
            cols = slice(nb * 512, nb * 512 + 512)
            rows = [dot_nn(p48[2 * q + k], dyall[q, k * TD:(k + 1) * TD, cols]) for k in range(2)]
            for i in range(NE):
                XQ[i, where, cols] = jnp.concatenate(
                    [weights[k][i][0:SL] * rows[k][i * SP:i * SP + SL] for k in range(2)], axis=0).astype(BF)
            for k in range(2):
                racc[k] = racc[k] + jnp.sum(rows[k] * YQ[2 * q + k, :, cols].astype(F32), axis=1, keepdims=True)
        for k in range(2):
            rh = hots[k] * racc[k]
            for i in range(NE):
                rloc[2 * q + k, i:i + 1, :] = jnp.sum(rh[i * SP:(i + 1) * SP], axis=0, keepdims=True)
        return 0

    lax.fori_loop(0, CH, gather, 0)
    for e in (3, 4):
        a_out(e).wait()
    for c in ycopies:
        c.wait_send()
    rsend = [remote(rloc, rall.at[me], rs.at[m - 1], rr.at[m - 1], me ^ m) for m in PEERS]
    out_Q = pltpu.make_async_copy(XQ, Q_hbm, osem.at[1])
    out_Q.start()

    def d_out(n):
        return pltpu.make_async_copy(DH.at[lax.rem(n, 2)], DH_hbm.at[NE - 1 - n], dsem.at[lax.rem(n, 2)])

    second = [remote(rab.at[0, 1], rcv2.at[0], qs.at[0], qr.at[0], me ^ 4),
              remote(rab.at[1, 1], rcv2.at[1], qs.at[1], qr.at[1], me ^ 2)]

    def expert_back(n, _):
        e = NE - 1 - n
        slot = lax.rem(e, 2)
        dslot = lax.rem(n, 2)

        @pl.when(n >= 2)
        def _():
            h_in(e).wait()
            d_out(n - 2).wait()

        da = dot_nt(XQ[e], wd[e])
        for b in range(4):
            lo = b * 256
            d = da[:, b * 128:b * 128 + 128]
            DHS[:, lo:lo + 128] = (d * h[slot, :, lo:lo + 128]).astype(BF)
            DHS[:, lo + 128:lo + 256] = (d * h[slot, :, lo + 128:lo + 256]).astype(BF)

        @pl.when(n < 3)
        def _():
            h_in(e - 2).start()

        prow = pl.ds(pl.multiple_of(e * SP, SP), SL)
        for b in range(3):
            cols = slice(b * 512, b * 512 + 512)
            p = dot_nt(DHS[...], wgu[e, cols, :])
            for q in range(ND):
                YQ[q, prow, cols] = p[q * SL:(q + 1) * SL].astype(BF)
        for b in range(4):
            cols = slice(b * 256, b * 256 + 256)
            DH[dslot, :, cols] = dot_nt(DHS[:, cols], perm[...]).astype(BF)
        d_out(n).start()

        @pl.when(n == 0)
        def _():
            for c in rsend:
                c.start()

        @pl.when(n == 2)
        def _():
            for m in range(2):
                first[m].wait_recv()
                rab[m, 1] = rab[m, 1] + rcvo[2 - m, :, m * HALF:(m + 1) * HALF]

        @pl.when(n == 3)
        def _():
            for c in second:
                c.start()

        return 0

    lax.fori_loop(0, NE, expert_back, 0)
    rall[me] = rloc[...]
    d_out(3).wait()
    d_out(4).wait()

    def combine_p(dev, cols):
        return dot_tn(p48[dev], YQ[dev, :, cols])

    pcopies = pair_copies(me, snd, rcvd, es, er)
    for n in range(CH):
        send_block(me, combine_p, snd, pcopies, n)
    outs = []
    places = ((sX.at[1], sY.at[1]), (sX.at[0], kb1), (ka1, sY.at[0]), (ka0, kb0))

    def finish_p(n):
        add_block(me, combine_p, rcvd, pcopies, n)
        if n == CH - 1:
            rcvd[n] = rcvd[n] + rdx
        for m, dst in enumerate(places[n]):
            o = pltpu.make_async_copy(rcvd.at[n, :, m * HALF:(m + 1) * HALF], dst, osem.at[2 + 2 * n + m])
            o.start()
            outs.append(o)

    for c in rsend:
        c.wait()
    pcopies[CH - 1].start()
    acc = jnp.zeros((EX, D), F32)
    accb = jnp.zeros((EX, 1), F32)
    for v in range(ND):
        w = wt[v]
        r = jnp.concatenate([rall[dv, v, 0:NE, :] for dv in range(ND)], axis=0)
        t = w * (r - jnp.sum(w * r, axis=0, keepdims=True))
        dl[v] = t.astype(BF)
        accb = accb + jnp.sum(t.astype(BF).astype(F32), axis=1, keepdims=True)
        acc = acc + dot_nn(dl[v], xall[v // 2, (v % 2) * TD:(v % 2) * TD + TD, :])
    gwr_out[...] = acc
    gbr_out[...] = jnp.broadcast_to(accb, (EX, 128))
    rdx = dot_tn(dl[me], wrt_ref[...])

    for n in range(CH):
        finish_p(n)
    for n in range(2):
        first[2 + n].wait_recv()
        second[n].wait()
        lanes = slice(n * HALF, n * HALF + HALF)
        out_ref[:, lanes] = (rab[n, 0] + rcvo[3, :, lanes] + rcv2[n]).astype(BF)
    for o in outs:
        o.wait()
    for c in pcopies:
        c.wait_send()
    out_Q.wait()
    for c in first:
        c.wait_send()
    gx.drain_sends()
    gy.drain_sends()


ORDER = (3, 1, 2, 0)


def pair_copies(me, snd, rcv, cs, cr):
    return [remote(snd.at[n], rcv.at[n], cs.at[n], cr.at[n], me ^ 1) for n in range(CH)]


def send_block(me, combine, snd, copies, n):
    for cols in THIRDS:
        snd[n, :, cols] = combine(me ^ 1 ^ (2 * ORDER[n]), cols)
    if n:
        copies[n - 1].start()


def add_block(me, combine, rcv, copies, n):
    vals = [combine(me ^ (2 * ORDER[n]), cols) for cols in THIRDS]
    copies[n].wait_recv()
    for cols, v in zip(THIRDS, vals):
        rcv[n, :, cols] = rcv[n, :, cols] + v


def weight_grad_kernel(passed, a_hbm, b_hbm, *refs):
    a_v, b_v, sem = refs[-3:]
    w_ref, s_ref = refs[passed:passed + 2]
    e, j = pl.program_id(0), pl.program_id(1)
    bm = w_ref.shape[1]

    def fetch(n):
        return (pltpu.make_async_copy(a_hbm.at[n], a_v.at[n], sem.at[0, n]),
                pltpu.make_async_copy(b_hbm.at[n], b_v.at[n], sem.at[1, n]))

    @pl.when((e == 0) & (j == 0))
    def _():
        for n in range(NE):
            for c in fetch(n):
                c.start()
        for n in range(passed):
            refs[passed + 2 + n][...] = refs[n][...]

    @pl.when(j == 0)
    def _():
        for c in fetch(e):
            c.wait()
        s_ref[pl.ds(e, 1), :] = jnp.sum(b_v[e].astype(F32), axis=0, keepdims=True)

    w_ref[0] = dot_tn(a_v[e, :, pl.ds(pl.multiple_of(j * bm, bm), bm)], b_v[e])


def weight_grad(a, b, nblk, passed=()):
    m, n = a.shape[2], b.shape[2]
    bm = m // nblk
    return pl.pallas_call(
        functools.partial(weight_grad_kernel, len(passed)),
        grid=(NE, nblk),
        in_specs=[pl.BlockSpec(memory_space=pltpu.HBM)] * 2 + [pl.BlockSpec(v.shape, lambda e, j: (0, 0)) for v in passed],
        out_specs=[pl.BlockSpec((1, bm, n), lambda e, j: (e, j, 0)), pl.BlockSpec((NE, n), lambda e, j: (0, 0)),
                   *[pl.BlockSpec(v.shape, lambda e, j: (0, 0)) for v in passed]],
        out_shape=[sds((NE, m, n), F32), sds((NE, n), F32), *[sds(v.shape, v.dtype) for v in passed]],
        scratch_shapes=[pltpu.VMEM(a.shape, BF), pltpu.VMEM(b.shape, BF), pltpu.SemaphoreType.DMA((2, NE))],
        compiler_params=pltpu.CompilerParams(vmem_limit_bytes=60 << 20),
        cost_estimate=pl.CostEstimate(flops=2 * NE * RE * m * n, bytes_accessed=4 * NE * m * n, transcendentals=0),
    )(a, b, *passed)


def last_kernel(ka, rx, a2, kb, ry, b2, out_ref):
    out_ref[:, 0:HALF] = (ka[...] + rx[0] + a2[...]).astype(BF)
    out_ref[:, HALF:D] = (kb[...] + ry[0] + b2[...]).astype(BF)


def sds(shape, dt):
    return jax.ShapeDtypeStruct(shape, dt)


def solution(mesh):
    perm_of = lambda m: [(i, i ^ m) for i in range(8)]
    hop_x, hop_y = perm_of(2), perm_of(4)
    DMA = pltpu.SemaphoreType.DMA
    part = sds((TD, HALF), F32)
    hops = sds((2, TD, HALF), F32)

    def local_block(hidden, grad_out, w_router, b_router, expert_ids, slot_ids, w_gate_up, b_gate_up, w_down, b_down):
        wrt = w_router.T
        outs = pl.pallas_call(
            block_kernel,
            in_specs=[ANY, ANY, ANY, ANY, VM, VM, VM, VM, ANY, ANY],
            out_specs=[ANY] * 11 + [VM] * 3,
            out_shape=[hops] * 2 + [part] * 4 + [
                sds((NE, RE, D), BF), sds((NE, RE, F), BF), sds((NE, RE, D), BF), sds((NE, RE, 2 * F), BF), sds((3, RE, 2 * F), F32),
                sds((EX, D), F32), sds((EX, 128), F32), sds((TD, D), BF)],
            scratch_shapes=[
                pltpu.VMEM((CH, 2 * TD, D), BF), pltpu.VMEM((CH, 2 * TD, D), BF), pltpu.VMEM((ND, 2 * TK, TD), jnp.int32),
                pltpu.VMEM((NE, D, 2 * F), BF), pltpu.VMEM((NE, F, D), BF), pltpu.VMEM((NE, RE, D), BF), pltpu.VMEM((ND, KC, D), BF),
                pltpu.VMEM((2, RE, 2 * F), F32), pltpu.VMEM((2, RE, F), BF), pltpu.VMEM((2, RE, 2 * F), BF), pltpu.VMEM((RE, 2 * F), BF),
                pltpu.VMEM((ND, KC, 3 * TD), BF), pltpu.VMEM((ND, KC, TD), BF), pltpu.VMEM((ND, EX, TD), F32),
                pltpu.VMEM((ND, 8, TD), F32), pltpu.VMEM((NE, 2 * F), F32),
                pltpu.VMEM((CH, TD, D), F32), pltpu.VMEM((CH, TD, D), F32), pltpu.VMEM((CH, TD, D), F32),
                pltpu.VMEM((2, 2, TD, HALF), F32), pltpu.VMEM((2, TD, HALF), F32), pltpu.VMEM((256, 256), BF),
                pltpu.VMEM((ND, 8, TD), F32), pltpu.VMEM((ND, ND, 8, TD), F32), pltpu.VMEM((ND, EX, TD), BF),
                DMA((4,)), DMA((2 * NE,)), DMA((4,)), DMA((2,)), DMA((2,)), DMA((10,)),
                *[DMA((10,))] * 4, *[DMA((7,))] * 2,
                *[DMA((CH,))] * 6, *[DMA((7,))] * 2, *[DMA((2,))] * 2],
            compiler_params=pltpu.CompilerParams(collective_id=0, has_side_effects=True, vmem_limit_bytes=VLIMIT),
            cost_estimate=pl.CostEstimate(flops=50_000_000_000, bytes_accessed=60_000_000, transcendentals=0),
        )(hidden, grad_out, expert_ids.T, slot_ids.T, wrt, b_router[None, :], b_gate_up, b_down, w_gate_up, w_down)
        sX, sY, ka0, ka1, kb0, kb1, X, A, Q, DH, _, gwr, gbr, block_out = outs
        rX = lax.ppermute(sX, 'ep', hop_x)
        rY = lax.ppermute(sY, 'ep', hop_y)
        gwgu, gbgu, block_out, gwr = weight_grad(X, DH, 2, (block_out, gwr))
        ka1, kb1, gbgu = lax.optimization_barrier((ka1, kb1, gbgu))
        ta = ka1 + rX[1]
        tb = kb1 + rY[1]
        ta, tb, A = lax.optimization_barrier((ta, tb, A))
        gwd, gbd = weight_grad(A, Q, 1)
        a2 = lax.ppermute(ta, 'ep', hop_y)
        b2 = lax.ppermute(tb, 'ep', hop_x)
        grad_hidden = pl.pallas_call(
            last_kernel, in_specs=[VM] * 6, out_specs=VM, out_shape=sds((TD, D), BF),
            compiler_params=pltpu.CompilerParams(vmem_limit_bytes=16 << 20),
        )(ka0, rX, a2, kb0, rY, b2)
        return (block_out, grad_hidden, gwr.T, gbr[:, 0], gwgu, gbgu, gwd, gbd)

    row = P('ep')
    in_specs = (row, row, P(), P(), row, row, row, row, row, row)
    out_specs = (row, row, P(), P(), row, row, row, row)
    return jax.shard_map(local_block, mesh=mesh, in_specs=in_specs, out_specs=out_specs, check_vma=False)
```

```python
import functools

import jax
import jax.numpy as jnp
from jax import lax
from jax.experimental import pallas as pl
from jax.experimental.pallas import tpu as pltpu
from jax.sharding import PartitionSpec as P

LIMIT = 7.0
ALPHA = 1.702

CH = 4
ND = 2 * CH
PEERS = range(1, ND)
EX = 40
NE = 5
TD = 128
D = 1536
F = 512
SL = 40
R2 = 2 * SL
HALF = D // 2
RE = CH * R2
SP = 48
KC = NE * SP
TK = 8
THIRDS = [slice(i, i + 512) for i in range(0, D, 512)]
BF = jnp.bfloat16
F32 = jnp.float32
ANY = pl.BlockSpec(memory_space=pl.ANY)
VM = pl.BlockSpec(memory_space=pltpu.VMEM)
VLIMIT = 67000000


def dot_nn(a, b):
    return lax.dot_general(a, b, (((1,), (0,)), ((), ())), preferred_element_type=F32)


def dot_nt(a, b):
    return lax.dot_general(a, b, (((1,), (1,)), ((), ())), preferred_element_type=F32)


def dot_tn(a, b):
    return lax.dot_general(a, b, (((0,), (0,)), ((), ())), preferred_element_type=F32)


def deinterleave_matrix():
    row = lax.broadcasted_iota(jnp.int32, (256, 256), 0)
    col = lax.broadcasted_iota(jnp.int32, (256, 256), 1)
    src = jnp.where(col < 128, 2 * col, 2 * col - 255)
    return jnp.where(row == src, 1.0, 0.0).astype(BF)


def entry_barrier(peers):
    barrier = pltpu.get_barrier_semaphore()
    for p in peers:
        pl.semaphore_signal(barrier, inc=1, device_id=(p,), device_id_type=pl.DeviceIdType.MESH)
    pl.semaphore_wait(barrier, len(peers))


def remote(src, dst, ssem, rsem, dev):
    return pltpu.make_async_remote_copy(src_ref=src, dst_ref=dst, send_sem=ssem, recv_sem=rsem,
                                        device_id=(dev,), device_id_type=pl.DeviceIdType.MESH)


class Gather:
    def __init__(self, me, own, buf, ssem, rsem):
        self.me, self.own, self.buf, self.ssem, self.rsem = me, own, buf, ssem, rsem

    def block(self, dev, lo=0, n=TD):
        core = lax.rem(dev, 2)
        return self.buf.at[dev // 2, pl.ds(pl.multiple_of(core * TD + lo, 64), n), :]

    def copy(self, slot, src, dst, dev):
        return remote(src, dst, self.ssem.at[slot], self.rsem.at[slot], dev)

    def descs(self):
        me = self.me
        c, x, y = me ^ 1, me ^ 2, me ^ 4
        own, blk, cp = self.own, self.block, self.copy
        self.x0 = cp(0, own.at[pl.ds(0, 64), :], blk(me, 0, 64), x)
        self.x1 = cp(1, own.at[pl.ds(64, 64), :], blk(me, 64, 64), x)
        self.y0 = cp(2, own.at[pl.ds(0, 64), :], blk(me, 0, 64), y)
        self.y1 = cp(3, own.at[pl.ds(64, 64), :], blk(me, 64, 64), y)
        self.d0 = cp(4, blk(x, 0, 64), blk(x, 0, 64), y)
        self.d1 = cp(5, blk(y, 64, 64), blk(y, 64, 64), x)
        self.c0 = cp(6, own, blk(me), c)
        self.c1 = cp(7, blk(x), blk(x), c)
        self.c2 = cp(8, blk(y), blk(y), c)
        self.c3 = cp(9, blk(me ^ 6), blk(me ^ 6), c)

    def start_own(self):
        self.descs()
        self.x0.start()
        self.y1.start()
        self.c0.start()
        self.x1.start()
        self.y0.start()

    def relay(self):
        self.x0.wait_recv()
        self.d0.start()
        self.y1.wait_recv()
        self.d1.start()

    def pair_xy(self):
        self.x1.wait_recv()
        self.c1.start()
        self.y0.wait_recv()
        self.c2.start()

    def pair_d(self):
        self.d0.wait_recv()
        self.d1.wait_recv()
        self.c3.start()

    def drain_sends(self):
        for d in (self.x0, self.x1, self.y0, self.y1, self.d0, self.d1, self.c0, self.c1, self.c2, self.c3):
            d.wait_send()


def split3(v):
    hi = v.astype(BF)
    r1 = v - hi.astype(F32)
    mid = r1.astype(BF)
    lo = (r1 - mid.astype(F32)).astype(BF)
    return hi, mid, lo


def block_kernel(x_hbm, dy_hbm, ids_hbm, slots_hbm, wrt_ref, br_ref, bgu_ref, bd_ref, wgu_hbm, wd_hbm,
                 sX, sY, ka0, ka1, kb0, kb1, X_hbm, A_hbm, Q_hbm, DH_hbm, h_hbm,
                 gwr_out, gbr_out, out_ref,
                 xall, dyall, meta, wgu, wd, XQ, YQ, h, A, DH, DHS, pw, p48, wt, wloc, bg,
                 snd, rcvo, rcvd, rab, rcv2, perm, rloc, rall, dl,
                 lsem, wsem, hsem, asem, dsem, osem, xs, xr, ds, dr, ms, mr, cs, cr, es, er, ps, pr, rs, rr, qs, qr):
    me = lax.axis_index('ep')
    chip = me // 2
    core = lax.rem(me, 2)
    mine_rows = pl.ds(pl.multiple_of(core * TD, TD), TD)
    own_m = [pltpu.make_async_copy(ids_hbm, meta.at[me, 0:TK, :], lsem.at[2]),
             pltpu.make_async_copy(slots_hbm, meta.at[me, TK:2 * TK, :], lsem.at[3])]
    own_x = pltpu.make_async_copy(x_hbm, xall.at[chip, mine_rows, :], lsem.at[0])
    own_dy = pltpu.make_async_copy(dy_hbm, dyall.at[chip, mine_rows, :], lsem.at[1])
    for c in own_m:
        c.start()
    own_x.start()
    own_dy.start()
    for e in range(NE):
        pltpu.make_async_copy(wgu_hbm.at[e], wgu.at[e], wsem.at[e]).start()
    entry_barrier([me ^ m for m in PEERS])
    gx = Gather(me, x_hbm, xall, xs, xr)
    gy = Gather(me, dy_hbm, dyall, ds, dr)
    gx.start_own()
    for c in own_m:
        c.wait()
    metas = [remote(meta.at[me], meta.at[me], ms.at[m - 1], mr.at[m - 1], me ^ m) for m in PEERS]
    for c in metas:
        c.start()
    for e in range(NE):
        pltpu.make_async_copy(wd_hbm.at[e], wd.at[e], wsem.at[NE + e]).start()
    perm[...] = deinterleave_matrix()
    YQ[...] = jnp.zeros_like(YQ)
    wloc[...] = jnp.zeros_like(wloc)
    rloc[...] = jnp.zeros_like(rloc)
    for b in range(4):
        cols = slice(b * 256, b * 256 + 256)
        bg[:, cols] = sum(dot_nn(part, perm[...]) for part in split3(bgu_ref[:, cols]))
    eye = lax.broadcasted_iota(jnp.int32, (EX, EX), 0) == lax.broadcasted_iota(jnp.int32, (EX, EX), 1)
    br_col = jnp.sum(jnp.where(eye, br_ref[...], 0.0), axis=1, keepdims=True)

    def permute(e):
        pltpu.make_async_copy(wgu_hbm.at[e], wgu.at[e], wsem.at[e]).wait()

        def body(b, _):
            cols = pl.ds(pl.multiple_of(b * 256, 256), 256)
            for r in range(3):
                rows = slice(r * 512, r * 512 + 512)
                wgu[e, rows, cols] = dot_nn(wgu[e, rows, cols], perm[...]).astype(BF)
            return 0

        lax.fori_loop(0, 4, body, 0)

    permute(0)
    permute(1)
    gx.relay()
    gy.start_own()
    permute(2)
    permute(3)
    own_x.wait()
    for c in metas:
        c.wait()
    permute(4)

    iota40 = lax.broadcasted_iota(jnp.int32, (EX, TD), 0)
    iota48 = lax.broadcasted_iota(jnp.int32, (SP, TD), 0)

    def route(q):
        lt = dot_nt(wrt_ref[...], xall[q]) + br_col
        for k in range(2):
            ids = meta[2 * q + k, 0:TK, :]
            slt = meta[2 * q + k, TK:2 * TK, :]
            slot = jnp.full((EX, TD), -1, jnp.int32)
            chosen = jnp.zeros((EX, TD), jnp.int32)
            for j in range(TK):
                hit = ids[j:j + 1, :] == iota40
                slot = jnp.where(hit, slt[j:j + 1, :], slot)
                chosen = jnp.where(hit, 1, chosen)
            on = chosen == 1
            lk = lt[:, k * TD:(k + 1) * TD]
            mx = jnp.max(jnp.where(on, lk, -jnp.inf), axis=0, keepdims=True)
            ex = jnp.where(on, jnp.exp(lk - mx), 0.0)
            w = ex / jnp.sum(ex, axis=0, keepdims=True)
            wt[2 * q + k] = w
            slotf = slot.astype(F32)
            for i in range(NE):
                mine = iota40 == me * NE + i
                s = jnp.max(jnp.where(mine, slotf, -1.0), axis=0, keepdims=True)
                wv = jnp.sum(jnp.where(mine, w, 0.0), axis=0, keepdims=True)
                hot = s.astype(jnp.int32) == iota48
                p48[2 * q + k, i * SP:(i + 1) * SP, :] = jnp.where(hot, 1.0, 0.0).astype(BF)
                for n, part in enumerate(split3(jnp.where(hot, wv, 0.0))):
                    pw[2 * q + k, i * SP:(i + 1) * SP, n * TD:(n + 1) * TD] = part
                wloc[2 * q + k, i:i + 1, :] = wv
        where = pl.ds(pl.multiple_of(q * R2, R2), R2)
        for nb in range(3):
            cols = slice(nb * 512, nb * 512 + 512)
            rows = [dot_nn(p48[2 * q + k], xall[q, k * TD:(k + 1) * TD, cols]) for k in range(2)]
            for i in range(NE):
                XQ[i, where, cols] = jnp.concatenate([r[i * SP:i * SP + SL] for r in rows], axis=0).astype(BF)

    gx.c0.wait_recv()
    route(chip)
    gx.pair_xy()
    gx.pair_d()
    gx.c1.wait_recv()
    gx.c2.wait_recv()

    def route_next(i, _):
        route(chip ^ i)
        return 0

    lax.fori_loop(1, 3, route_next, 0)
    gx.c3.wait_recv()
    route(chip ^ 3)
    out_X = pltpu.make_async_copy(XQ, X_hbm, osem.at[0])
    out_X.start()

    def h_out(e):
        return pltpu.make_async_copy(h.at[lax.rem(e, 2)], h_hbm.at[e], hsem.at[lax.rem(e, 2)])

    def h_in(e):
        return pltpu.make_async_copy(h_hbm.at[e], h.at[lax.rem(e, 2)], hsem.at[2 + lax.rem(e, 2)])

    def a_out(e):
        return pltpu.make_async_copy(A.at[lax.rem(e, 2)], A_hbm.at[e], asem.at[lax.rem(e, 2)])

    def expert(e, _):
        slot = lax.rem(e, 2)

        @pl.when(e >= 2)
        def _():
            h_out(e - 2).wait()
            a_out(e - 2).wait()

        for b in range(4):
            cols = slice(b * 256, b * 256 + 256)
            pre = dot_nn(XQ[e], wgu[e, :, cols]) + bg[pl.ds(e, 1), cols]
            hg, hu = pre[:, :128], pre[:, 128:]
            g = jnp.minimum(hg, LIMIT)
            u1 = jnp.clip(hu, -LIMIT, LIMIT) + 1.0
            sg = jax.nn.sigmoid(ALPHA * g)
            gs = g * sg
            A[slot, :, b * 128:b * 128 + 128] = (gs * u1).astype(BF)
            au = jnp.abs(hu)
            mg = jnp.where(hg < LIMIT, 1.0, jnp.where(hg == LIMIT, 0.5, 0.0))
            mu = jnp.where(au < LIMIT, 1.0, jnp.where(au == LIMIT, 0.5, 0.0))
            h[slot, :, b * 256:b * 256 + 128] = u1 * (sg + ALPHA * gs * (1.0 - sg)) * mg
            h[slot, :, b * 256 + 128:b * 256 + 256] = gs * mu
        a_out(e).start()

        @pl.when(e < 3)
        def _():
            h_out(e).start()

        pltpu.make_async_copy(wd_hbm.at[e], wd.at[e], wsem.at[NE + e]).wait()
        yrow = pl.ds(pl.multiple_of(e * SP, SP), SL)
        for b in range(3):
            cols = slice(b * 512, b * 512 + 512)
            y = dot_nn(A[slot], wd[e, :, cols]) + bd_ref[pl.ds(e, 1), cols]
            for q in range(ND):
                YQ[q, yrow, cols] = y[q * SL:(q + 1) * SL].astype(BF)

        @pl.when(e == 0)
        def _():
            gy.relay()

        @pl.when(e == 2)
        def _():
            gy.pair_xy()

        return 0

    lax.fori_loop(0, NE, expert, 0)

    def combine_y(dev, cols):
        full = dot_tn(pw[dev], YQ[dev, :, cols])
        return full[0:TD] + full[TD:2 * TD] + full[2 * TD:3 * TD]

    first = [remote(rcvo.at[0, :, 0:HALF], rab.at[0, 1], ps.at[0], pr.at[0], me ^ 2),
             remote(rcvo.at[0, :, HALF:D], rab.at[1, 1], ps.at[1], pr.at[1], me ^ 4),
             remote(rcvo.at[1, :, 0:HALF], rab.at[0, 0], ps.at[2], pr.at[2], me ^ 2),
             remote(rcvo.at[2, :, HALF:D], rab.at[1, 0], ps.at[3], pr.at[3], me ^ 4)]

    ycopies = pair_copies(me, snd, rcvo, cs, cr)
    for n in range(CH - 1):
        send_block(me, combine_y, snd, ycopies, n)
    add_block(me, combine_y, rcvo, ycopies, 0)
    send_block(me, combine_y, snd, ycopies, 3)
    first[0].start()
    first[1].start()
    ycopies[CH - 1].start()
    add_block(me, combine_y, rcvo, ycopies, 1)
    add_block(me, combine_y, rcvo, ycopies, 2)
    first[2].start()
    gy.pair_d()
    add_block(me, combine_y, rcvo, ycopies, 3)
    first[3].start()

    gy.c0.wait_recv()
    gy.c1.wait_recv()
    gy.c2.wait_recv()
    gy.c3.wait_recv()
    own_dy.wait()
    out_X.wait()

    def gather(q, _):
        weights, hots, racc = [], [], []
        for k in range(2):
            hot = p48[2 * q + k].astype(F32)
            hots.append(hot)
            weights.append([jnp.sum(hot[i * SP:(i + 1) * SP] * wloc[2 * q + k, i:i + 1, :], axis=1, keepdims=True)
                            for i in range(NE)])
            racc.append(jnp.zeros((KC, 1), F32))
        where = pl.ds(pl.multiple_of(q * R2, R2), R2)
        for nb in range(3):
            cols = slice(nb * 512, nb * 512 + 512)
            rows = [dot_nn(p48[2 * q + k], dyall[q, k * TD:(k + 1) * TD, cols]) for k in range(2)]
            for i in range(NE):
                XQ[i, where, cols] = jnp.concatenate(
                    [weights[k][i][0:SL] * rows[k][i * SP:i * SP + SL] for k in range(2)], axis=0).astype(BF)
            for k in range(2):
                racc[k] = racc[k] + jnp.sum(rows[k] * YQ[2 * q + k, :, cols].astype(F32), axis=1, keepdims=True)
        for k in range(2):
            rh = hots[k] * racc[k]
            for i in range(NE):
                rloc[2 * q + k, i:i + 1, :] = jnp.sum(rh[i * SP:(i + 1) * SP], axis=0, keepdims=True)
        return 0

    lax.fori_loop(0, CH, gather, 0)
    for e in (3, 4):
        a_out(e).wait()
    for c in ycopies:
        c.wait_send()
    rsend = [remote(rloc, rall.at[me], rs.at[m - 1], rr.at[m - 1], me ^ m) for m in PEERS]
    out_Q = pltpu.make_async_copy(XQ, Q_hbm, osem.at[1])
    out_Q.start()

    def d_out(n):
        return pltpu.make_async_copy(DH.at[lax.rem(n, 2)], DH_hbm.at[NE - 1 - n], dsem.at[lax.rem(n, 2)])

    second = [remote(rab.at[0, 1], rcv2.at[0], qs.at[0], qr.at[0], me ^ 4),
              remote(rab.at[1, 1], rcv2.at[1], qs.at[1], qr.at[1], me ^ 2)]

    def expert_back(n, _):
        e = NE - 1 - n
        slot = lax.rem(e, 2)
        dslot = lax.rem(n, 2)

        @pl.when(n >= 2)
        def _():
            h_in(e).wait()
            d_out(n - 2).wait()

        da = dot_nt(XQ[e], wd[e])
        for b in range(4):
            lo = b * 256
            d = da[:, b * 128:b * 128 + 128]
            DHS[:, lo:lo + 128] = (d * h[slot, :, lo:lo + 128]).astype(BF)
            DHS[:, lo + 128:lo + 256] = (d * h[slot, :, lo + 128:lo + 256]).astype(BF)

        @pl.when(n < 3)
        def _():
            h_in(e - 2).start()

        prow = pl.ds(pl.multiple_of(e * SP, SP), SL)
        for b in range(3):
            cols = slice(b * 512, b * 512 + 512)
            p = dot_nt(DHS[...], wgu[e, cols, :])
            for q in range(ND):
                YQ[q, prow, cols] = p[q * SL:(q + 1) * SL].astype(BF)
        for b in range(4):
            cols = slice(b * 256, b * 256 + 256)
            DH[dslot, :, cols] = dot_nt(DHS[:, cols], perm[...]).astype(BF)
        d_out(n).start()

        @pl.when(n == 0)
        def _():
            for c in rsend:
                c.start()

        @pl.when(n == 2)
        def _():
            for m in range(2):
                first[m].wait_recv()
                rab[m, 1] = rab[m, 1] + rcvo[2 - m, :, m * HALF:(m + 1) * HALF]

        @pl.when(n == 3)
        def _():
            for c in second:
                c.start()

        return 0

    lax.fori_loop(0, NE, expert_back, 0)
    rall[me] = rloc[...]
    d_out(3).wait()
    d_out(4).wait()

    def combine_p(dev, cols):
        return dot_tn(p48[dev], YQ[dev, :, cols])

    pcopies = pair_copies(me, snd, rcvd, es, er)
    for n in range(CH):
        send_block(me, combine_p, snd, pcopies, n)
    outs = []
    places = ((sX.at[1], sY.at[1]), (sX.at[0], kb1), (ka1, sY.at[0]), (ka0, kb0))

    def finish_p(n):
        add_block(me, combine_p, rcvd, pcopies, n)
        if n == CH - 1:
            rcvd[n] = rcvd[n] + rdx
        for m, dst in enumerate(places[n]):
            o = pltpu.make_async_copy(rcvd.at[n, :, m * HALF:(m + 1) * HALF], dst, osem.at[2 + 2 * n + m])
            o.start()
            outs.append(o)

    for c in rsend:
        c.wait()
    pcopies[CH - 1].start()
    acc = jnp.zeros((EX, D), F32)
    accb = jnp.zeros((EX, 1), F32)
    for v in range(ND):
        w = wt[v]
        r = jnp.concatenate([rall[dv, v, 0:NE, :] for dv in range(ND)], axis=0)
        t = w * (r - jnp.sum(w * r, axis=0, keepdims=True))
        dl[v] = t.astype(BF)
        accb = accb + jnp.sum(t.astype(BF).astype(F32), axis=1, keepdims=True)
        acc = acc + dot_nn(dl[v], xall[v // 2, (v % 2) * TD:(v % 2) * TD + TD, :])
    gwr_out[...] = acc
    gbr_out[...] = jnp.broadcast_to(accb, (EX, 128))
    rdx = dot_tn(dl[me], wrt_ref[...])

    for n in range(CH):
        finish_p(n)
    for n in range(2):
        first[2 + n].wait_recv()
        second[n].wait()
        lanes = slice(n * HALF, n * HALF + HALF)
        out_ref[:, lanes] = (rab[n, 0] + rcvo[3, :, lanes] + rcv2[n]).astype(BF)
    for o in outs:
        o.wait()
    for c in pcopies:
        c.wait_send()
    out_Q.wait()
    for c in first:
        c.wait_send()
    gx.drain_sends()
    gy.drain_sends()


ORDER = (3, 1, 2, 0)


def pair_copies(me, snd, rcv, cs, cr):
    return [remote(snd.at[n], rcv.at[n], cs.at[n], cr.at[n], me ^ 1) for n in range(CH)]


def send_block(me, combine, snd, copies, n):
    for cols in THIRDS:
        snd[n, :, cols] = combine(me ^ 1 ^ (2 * ORDER[n]), cols)
    if n:
        copies[n - 1].start()


def add_block(me, combine, rcv, copies, n):
    vals = [combine(me ^ (2 * ORDER[n]), cols) for cols in THIRDS]
    copies[n].wait_recv()
    for cols, v in zip(THIRDS, vals):
        rcv[n, :, cols] = rcv[n, :, cols] + v


def weight_grad_kernel(passed, a_hbm, b_hbm, *refs):
    a_v, b_v, sem = refs[-3:]
    w_ref, s_ref = refs[passed:passed + 2]
    e, j = pl.program_id(0), pl.program_id(1)
    bm = w_ref.shape[1]

    def fetch(n):
        return (pltpu.make_async_copy(a_hbm.at[n], a_v.at[n], sem.at[0, n]),
                pltpu.make_async_copy(b_hbm.at[n], b_v.at[n], sem.at[1, n]))

    @pl.when((e == 0) & (j == 0))
    def _():
        for n in range(NE):
            for c in fetch(n):
                c.start()
        for n in range(passed):
            refs[passed + 2 + n][...] = refs[n][...]

    @pl.when(j == 0)
    def _():
        for c in fetch(e):
            c.wait()
        s_ref[pl.ds(e, 1), :] = jnp.sum(b_v[e].astype(F32), axis=0, keepdims=True)

    w_ref[0] = dot_tn(a_v[e, :, pl.ds(pl.multiple_of(j * bm, bm), bm)], b_v[e])


def weight_grad(a, b, nblk, passed=()):
    m, n = a.shape[2], b.shape[2]
    bm = m // nblk
    return pl.pallas_call(
        functools.partial(weight_grad_kernel, len(passed)),
        grid=(NE, nblk),
        in_specs=[pl.BlockSpec(memory_space=pltpu.HBM)] * 2 + [pl.BlockSpec(v.shape, lambda e, j: (0, 0)) for v in passed],
        out_specs=[pl.BlockSpec((1, bm, n), lambda e, j: (e, j, 0)), pl.BlockSpec((NE, n), lambda e, j: (0, 0)),
                   *[pl.BlockSpec(v.shape, lambda e, j: (0, 0)) for v in passed]],
        out_shape=[sds((NE, m, n), F32), sds((NE, n), F32), *[sds(v.shape, v.dtype) for v in passed]],
        scratch_shapes=[pltpu.VMEM(a.shape, BF), pltpu.VMEM(b.shape, BF), pltpu.SemaphoreType.DMA((2, NE))],
        compiler_params=pltpu.CompilerParams(vmem_limit_bytes=60 << 20),
        cost_estimate=pl.CostEstimate(flops=2 * NE * RE * m * n, bytes_accessed=4 * NE * m * n, transcendentals=0),
    )(a, b, *passed)


def last_kernel(ka, rx, a2, kb, ry, b2, out_ref):
    out_ref[:, 0:HALF] = (ka[...] + rx[0] + a2[...]).astype(BF)
    out_ref[:, HALF:D] = (kb[...] + ry[0] + b2[...]).astype(BF)


def sds(shape, dt):
    return jax.ShapeDtypeStruct(shape, dt)


def solution(mesh):
    perm_of = lambda m: [(i, i ^ m) for i in range(8)]
    hop_x, hop_y = perm_of(2), perm_of(4)
    DMA = pltpu.SemaphoreType.DMA
    part = sds((TD, HALF), F32)
    hops = sds((2, TD, HALF), F32)

    def local_block(hidden, grad_out, w_router, b_router, expert_ids, slot_ids, w_gate_up, b_gate_up, w_down, b_down):
        wrt = w_router.T
        outs = pl.pallas_call(
            block_kernel,
            in_specs=[ANY, ANY, ANY, ANY, VM, VM, VM, VM, ANY, ANY],
            out_specs=[ANY] * 11 + [VM] * 3,
            out_shape=[hops] * 2 + [part] * 4 + [
                sds((NE, RE, D), BF), sds((NE, RE, F), BF), sds((NE, RE, D), BF), sds((NE, RE, 2 * F), BF), sds((3, RE, 2 * F), F32),
                sds((EX, D), F32), sds((EX, 128), F32), sds((TD, D), BF)],
            scratch_shapes=[
                pltpu.VMEM((CH, 2 * TD, D), BF), pltpu.VMEM((CH, 2 * TD, D), BF), pltpu.VMEM((ND, 2 * TK, TD), jnp.int32),
                pltpu.VMEM((NE, D, 2 * F), BF), pltpu.VMEM((NE, F, D), BF), pltpu.VMEM((NE, RE, D), BF), pltpu.VMEM((ND, KC, D), BF),
                pltpu.VMEM((2, RE, 2 * F), F32), pltpu.VMEM((2, RE, F), BF), pltpu.VMEM((2, RE, 2 * F), BF), pltpu.VMEM((RE, 2 * F), BF),
                pltpu.VMEM((ND, KC, 3 * TD), BF), pltpu.VMEM((ND, KC, TD), BF), pltpu.VMEM((ND, EX, TD), F32),
                pltpu.VMEM((ND, 8, TD), F32), pltpu.VMEM((NE, 2 * F), F32),
                pltpu.VMEM((CH, TD, D), F32), pltpu.VMEM((CH, TD, D), F32), pltpu.VMEM((CH, TD, D), F32),
                pltpu.VMEM((2, 2, TD, HALF), F32), pltpu.VMEM((2, TD, HALF), F32), pltpu.VMEM((256, 256), BF),
                pltpu.VMEM((ND, 8, TD), F32), pltpu.VMEM((ND, ND, 8, TD), F32), pltpu.VMEM((ND, EX, TD), BF),
                DMA((4,)), DMA((2 * NE,)), DMA((4,)), DMA((2,)), DMA((2,)), DMA((10,)),
                *[DMA((10,))] * 4, *[DMA((7,))] * 2,
                *[DMA((CH,))] * 6, *[DMA((7,))] * 2, *[DMA((2,))] * 2],
            compiler_params=pltpu.CompilerParams(collective_id=0, has_side_effects=True, vmem_limit_bytes=VLIMIT),
            cost_estimate=pl.CostEstimate(flops=50_000_000_000, bytes_accessed=60_000_000, transcendentals=0),
        )(hidden, grad_out, expert_ids.T, slot_ids.T, wrt, b_router[None, :], b_gate_up, b_down, w_gate_up, w_down)
        sX, sY, ka0, ka1, kb0, kb1, X, A, Q, DH, _, gwr, gbr, block_out = outs
        rX = lax.ppermute(sX, 'ep', hop_x)
        rY = lax.ppermute(sY, 'ep', hop_y)
        gwgu, gbgu, block_out, gwr = weight_grad(X, DH, 1, (block_out, gwr))
        ka1, kb1, gbgu = lax.optimization_barrier((ka1, kb1, gbgu))
        ta = ka1 + rX[1]
        tb = kb1 + rY[1]
        ta, tb, A = lax.optimization_barrier((ta, tb, A))
        gwd, gbd = weight_grad(A, Q, 1)
        a2 = lax.ppermute(ta, 'ep', hop_y)
        b2 = lax.ppermute(tb, 'ep', hop_x)
        grad_hidden = pl.pallas_call(
            last_kernel, in_specs=[VM] * 6, out_specs=VM, out_shape=sds((TD, D), BF),
            compiler_params=pltpu.CompilerParams(vmem_limit_bytes=16 << 20),
        )(ka0, rX, a2, kb0, rY, b2)
        return (block_out, grad_hidden, gwr.T, gbr[:, 0], gwgu, gbgu, gwd, gbd)

    row = P('ep')
    in_specs = (row, row, P(), P(), row, row, row, row, row, row)
    out_specs = (row, row, P(), P(), row, row, row, row)
    return jax.shard_map(local_block, mesh=mesh, in_specs=in_specs, out_specs=out_specs, check_vma=False)
```
